32 devices in a mesh: dp: 16 (over z, y, core), rep: 2 (over x).
Axes of the slice: x: 2, y: 2, z: 4, core: 2. Of those that a mesh axis runs over, the one named last changes fastest.
Arguments:
- gate_pre: bfloat16 [2, 2048, 5632], P(None, 'dp', 'rep'), may hold values from -8 to 8
- up_pre: bfloat16 [2, 2048, 5632], P(None, 'dp', 'rep'), may hold values from -6 to 6
- out_grad: bfloat16 [2, 2048, 1024], P(None, 'dp'), may hold values from -6 to 6
- master: float32 [1024, 5632], P('dp', 'rep'), may hold values from -0.078125 to 0.078125
- moment_one: float32 [1024, 5632], P('dp', 'rep'), may hold values from -0.02 to 0.02
- moment_two: float32 [1024, 5632], P('dp', 'rep'), may hold values from 1e-06 to 1e-05
Outputs:
- layer_out: bfloat16 [2, 2048, 1024], P(None, 'dp', 'rep')
- gate_grad: bfloat16 [2, 2048, 5632], P(None, 'dp', 'rep')
- up_grad: bfloat16 [2, 2048, 5632], P(None, 'dp', 'rep')
- master_new: float32 [1024, 5632], P('dp', 'rep')
- moment_one_new: float32 [1024, 5632], P('dp', 'rep')
- moment_two_new: float32 [1024, 5632], P('dp', 'rep')
The draws below stay inside these ranges and needn't reach their ends.
All inputs are finite; a program needn't handle non-finite values.
Results may differ from the reference program's by a relative error of at most 0.0048.
The reference program's roundings to bfloat16 on the way (of `weight_bf` and `hidden`) count: a program that leaves them out, or rounds other values in their place, can miss the bound.
Values may be sent and summed in bfloat16 or wider, within the bound.
A program may use at most 128 MiB of HBM per device.

```python
import math
import jax
import jax.numpy as jnp
from jax import lax

D = 1024
FF = 5632
MB = 2
TOKENS = 2048


def strengthened(values, stream_key, source, target, shards_of, factor):
    def block_of(axis_at):
        return (jnp.arange(values.shape[axis_at]) // (values.shape[axis_at] // shards_of)).reshape((-1,) + (1,) * (values.ndim - 1 - axis_at))

    one_side = jax.random.permutation(stream_key, shards_of)[block_of(target)]
    far = (block_of(target) + shards_of // 2) % shards_of
    return jnp.where((block_of(source) == one_side) | (block_of(source) == far), factor * values, values)


def shard_levels(rng, shape, pieces, smallest, top_value):
    level, own = 1.0, jax.random.fold_in(rng, 6)
    for axis_at, blocks in pieces:
        draws = jnp.exp(jax.random.uniform(jax.random.fold_in(own, axis_at), (blocks,), jnp.float32, smallest / len(pieces), top_value / len(pieces)))
        level = level * jnp.repeat(draws, shape[axis_at] // blocks).reshape([-1 if axis == axis_at else 1 for axis in range(len(shape))])
    return level


def centred(rng, extent, width, most, pieces=(), held_as=jnp.bfloat16):
    array = jax.random.normal(rng, extent, jnp.float32) * width
    if len(pieces) > 0:
        array = shard_levels(rng, extent, pieces, -0.22, 0.18) * array
    return jnp.clip(array, min=-most, max=most).astype(held_as)


def heavy_noise(key, shape, scale, reach, pieces, heavy, dtype=jnp.bfloat16):
    drawn = scale * jax.random.normal(key, shape, jnp.float32)
    if pieces:
        drawn = drawn * shard_levels(key, shape, pieces, -0.22, 0.18)
    return jnp.clip(strengthened(drawn, jax.random.fold_in(key, 3), *heavy), -reach, reach).astype(dtype)


def setup_inputs(seed: int = 0) -> dict:
    splits = jax.random.split(jax.random.key(seed), 7)
    gate_pre = centred(splits[0], (MB, TOKENS, FF), 1.5, 8.0, ((1, 16), (2, 2)))
    up_pre = centred(splits[1], (MB, TOKENS, FF), 1.0, 6.0, ((1, 16), (2, 2)))
    out_grad = heavy_noise(splits[2], (MB, TOKENS, D), 1.0, 6.0, ((1, 16),), (1, 2, 16, 2.0))
    master = centred(splits[3], (D, FF), FF ** -0.5, 0.078125, ((0, 16), (1, 2)), jnp.float32)
    moment_one = centred(splits[4], (D, FF), 0.003, 0.02, ((0, 16), (1, 2)), jnp.float32)
    moment_two = jnp.clip(jnp.exp(math.log(9.999999747378752e-06) - 2.3025851 * jax.random.uniform(splits[5], (D, FF), jnp.float32) ** shard_levels(splits[5], (D, FF), ((0, 16), (1, 2)), -0.2, 0.2)), 9.999999974752427e-07, 9.999999747378752e-06)
    return {"gate_pre": gate_pre, "up_pre": up_pre, "out_grad": out_grad, "master": master, "moment_one": moment_one, "moment_two": moment_two}


first_power = 2.6561398887587544e-05
second_power = 0.005920529220333997

def reference(gate_pre, up_pre, out_grad, master, moment_one, moment_two):
    weight_bf = master.astype(jnp.bfloat16)
    outs_list = []
    gate_list = []
    up_list = []
    grad_sum = jnp.zeros(master.shape, jnp.float32)
    for index in range(MB):
        gate = gate_pre[index].astype(jnp.float32)
        up_val = up_pre[index].astype(jnp.float32)
        sig = jax.nn.sigmoid(gate)
        hidden = (gate * sig * up_val).astype(jnp.bfloat16)
        result = lax.dot_general(hidden, weight_bf, (((1,), (1,)), ((), ())), preferred_element_type=jnp.float32)
        outs_list.append(result.astype(jnp.bfloat16))
        hid_grad = jnp.dot(out_grad[index], weight_bf, preferred_element_type=jnp.float32)
        gate_list.append((hid_grad * up_val * sig * (1.0 + gate * (1.0 - sig))).astype(jnp.bfloat16))
        up_list.append((hid_grad * gate * sig).astype(jnp.bfloat16))
        grad_sum = grad_sum + lax.dot_general(out_grad[index], hidden, (((0,), (0,)), ((), ())), preferred_element_type=jnp.float32)
    main_grad = grad_sum / jnp.float32(MB * TOKENS)
    first = 0.9 * moment_one + 0.1 * main_grad
    second = 0.95 * moment_two + 0.05 * main_grad * main_grad
    update = first / (1.0 - first_power) / (jnp.sqrt(second / (1.0 - second_power)) + 1e-08)
    master_new = master - 0.003 * (update + 0.1 * master)
    return (jnp.stack(outs_list), jnp.stack(gate_list), jnp.stack(up_list), master_new, first, second)
```

```python
import functools

import jax
import jax.numpy as jnp
from jax import lax
from jax.experimental import pallas as pl
from jax.experimental.pallas import tpu as pltpu
from jax.sharding import PartitionSpec as P

first_power = 2.6561398887587544e-05
second_power = 0.005920529220333997

MESH = pl.DeviceIdType.MESH
CORES = 2
MID = 2


def adam(main_grad, master, moment_one, moment_two):
    first = 0.9 * moment_one + 0.1 * main_grad
    second = 0.95 * moment_two + 0.05 * main_grad * main_grad
    update = first / (1.0 - first_power) / (jnp.sqrt(second / (1.0 - second_power)) + 1e-08)
    return master - 0.003 * (update + 0.1 * master), first, second


def fused(
    outer, total,
    gate_hbm, up_hbm, cot_ref, master_ref, one_hbm, two_hbm,
    out_ref, gate_grad_ref, up_grad_ref, master_new_ref, first_ref, second_ref,
    weights, hid, hid_peer, cot_peer, own_sum, mid_send, mid_recv, outer_send, outer_recv,
    part_send, part_recv, cot_rows_ref, gate_ref, up_ref, one_ref, two_ref, local_sem,
    w_recv, w_mid_send, w_outer_send, w_core_send,
    core_send_sem, core_recv_sem,
    mid_send_sem, mid_recv_sem, outer_send_sem, outer_recv_sem, part_send_sem, part_recv_sem,
):
    me = lax.axis_index("dp")
    rep = lax.axis_index("rep")
    core = lax.rem(me, CORES)
    mid = lax.rem(me // CORES, MID)
    out = me // (CORES * MID)
    n = outer * MID * CORES
    rows, ff = master_ref.shape
    tokens = gate_ref.shape[0]
    loads = [
        pltpu.make_async_copy(src, dst, local_sem.at[index])
        for index, (src, dst) in enumerate(
            ((gate_hbm, gate_ref), (up_hbm, up_ref), (one_hbm, one_ref), (two_hbm, two_ref))
        )
    ]
    for load in loads:
        load.start()
    width = 256 if ff % 256 == 0 else 128
    chunks = ff // width

    def at(o, m, c):
        return (o * MID + m) * CORES + c

    core_peer = {"dp": at(out, mid, 1 - core)}
    mid_peer = {"dp": at(out, 1 - mid, core)}
    rep_peer = {"rep": 1 - rep}

    def outer_at(k):
        return lax.rem(out + k, outer)

    def outer_peer(k):
        return {"dp": at(outer_at(k), mid, core)}

    def remote(src, dst, send, recv, device):
        return pltpu.make_async_remote_copy(
            src_ref=src, dst_ref=dst, send_sem=send, recv_sem=recv,
            device_id=device, device_id_type=MESH,
        )

    weights[me] = master_ref[...].astype(jnp.bfloat16)
    barrier = pltpu.get_barrier_semaphore()
    peers = [core_peer, mid_peer, rep_peer] + [outer_peer(k) for k in range(1, outer)]
    for peer in peers:
        pl.semaphore_signal(barrier, inc=1, device_id=peer, device_id_type=MESH)
    pl.semaphore_wait(barrier, len(peers))

    order = sorted(range(1, outer), key=lambda k: min(k, outer - k))
    started = []

    def go(copy):
        copy.start()
        started.append(copy)
        return copy

    for k in order:
        go(remote(weights.at[me], weights.at[me], w_outer_send.at[k], w_recv.at[me], outer_peer(k)))
    go(remote(weights.at[me], weights.at[me], w_mid_send.at[0], w_recv.at[me], mid_peer))
    go(remote(weights.at[me], weights.at[me], w_core_send.at[0], w_recv.at[me], core_peer))
    turned = jnp.transpose(cot_ref[...].astype(jnp.float32)).astype(jnp.bfloat16).reshape(n, rows, tokens)
    for o in range(outer):
        for m in range(MID):
            for c in range(CORES):
                cot_rows_ref[c, m, o] = turned[at(o, m, c)]
    loads[0].wait()
    loads[1].wait()

    def columns(j):
        return pl.ds(pl.multiple_of(j * width, width), width)

    def hidden_step(j, carry):
        cols = columns(j)
        gate = gate_ref[:, cols].astype(jnp.float32)
        sig = jax.nn.sigmoid(gate)
        hid[:, cols] = (gate * sig * up_ref[:, cols].astype(jnp.float32)).astype(jnp.bfloat16)
        return carry

    lax.fori_loop(0, chunks, hidden_step, 0)
    cot_copy = go(remote(cot_rows_ref.at[1 - core], cot_peer, core_send_sem.at[0], core_recv_sem.at[0], core_peer))
    hid_copy = go(remote(hid, hid_peer, core_send_sem.at[1], core_recv_sem.at[1], core_peer))
    cot_copy.wait_recv()
    hid_copy.wait_recv()

    def grad_of(which, cols):
        own = cot_rows_ref[core, which].reshape(outer * rows, tokens)
        other = cot_peer[which].reshape(outer * rows, tokens)
        value = jnp.dot(own, hid[:, cols], preferred_element_type=jnp.float32)
        value += jnp.dot(other, hid_peer[:, cols], preferred_element_type=jnp.float32)
        return value.reshape(outer, rows, width)

    def send_step(j, carry):
        cols = columns(j)
        mid_send[:, :, cols] = grad_of(1 - mid, cols).astype(jnp.bfloat16)
        return carry

    lax.fori_loop(0, chunks, send_step, 0)

    def reduce_mid(k):
        slot = outer_at(k)
        go(remote(mid_send.at[slot], mid_recv.at[slot], mid_send_sem.at[k], mid_recv_sem.at[slot], mid_peer))

    def arrival(slot):
        return remote(weights.at[slot], weights.at[slot], w_core_send.at[0], w_recv.at[slot], core_peer)

    def forward_outer(k):
        slot = at(lax.rem(out + outer - k, outer), mid, core)
        arrival(slot).wait_recv()
        go(remote(weights.at[slot], weights.at[slot], w_mid_send.at[k], w_recv.at[slot], mid_peer))
        go(remote(weights.at[slot], weights.at[slot], w_core_send.at[k], w_recv.at[slot], core_peer))

    def forward_mid(k):
        slot = at(lax.rem(out + outer - k, outer), 1 - mid, core)
        arrival(slot).wait_recv()
        go(remote(weights.at[slot], weights.at[slot], w_core_send.at[outer + k], w_recv.at[slot], core_peer))

    def mid_wait(slot):
        remote(mid_recv.at[slot], mid_recv.at[slot], mid_send_sem.at[0], mid_recv_sem.at[slot], mid_peer).wait_recv()

    def pass_on(k):
        slot = outer_at(k)
        mid_wait(slot)

        def step(j, carry):
            cols = columns(j)
            outer_send[slot, :, cols] = (
                own_sum[slot, :, cols] + mid_recv[slot, :, cols].astype(jnp.float32)
            ).astype(jnp.bfloat16)
            return carry

        lax.fori_loop(0, chunks, step, 0)
        go(remote(outer_send.at[slot], outer_recv.at[out], outer_send_sem.at[k], outer_recv_sem.at[out], outer_peer(k)))

    back = list(reversed(order))
    forward_outer(order[0])
    reduce_mid(back[0])
    def own_step(j, carry):
        cols = columns(j)
        own_sum[:, :, cols] = grad_of(mid, cols)
        return carry

    lax.fori_loop(0, chunks, own_step, 0)

    forward_mid(0)
    for index in range(1, outer - 1):
        forward_outer(order[index])
        reduce_mid(back[index])
        if index < outer - 2:
            pass_on(back[index - 1])
    reduce_mid(0)
    for k in order[:-1]:
        forward_mid(k)
    if outer > 2:
        pass_on(back[-2])
    forward_mid(order[-1])
    for k in range(outer):
        for m in range(MID):
            arrival(at(outer_at(k), m, 1 - core)).wait_recv()

    half = n // 2
    group = max(1, min(half, 256 // rows))

    def part_step(base, target):
        def step(g, carry):
            some = weights[pl.ds(base + g * group, group)].reshape(group * rows, ff)
            target[g] = lax.dot_general(
                hid[...], some, (((1,), (1,)), ((), ())), preferred_element_type=jnp.float32
            )
            return carry

        lax.fori_loop(0, half // group, step, 0)

    part_step((1 - rep) * half, part_send)
    part_copy = go(remote(part_send, part_recv, part_send_sem, part_recv_sem, rep_peer))

    def input_step(j, carry):
        cols = columns(j)
        grad = jnp.dot(
            cot_ref[...], weights[:, :, cols].reshape(n * rows, width),
            preferred_element_type=jnp.float32,
        )
        gate = gate_ref[:, cols].astype(jnp.float32)
        up_val = up_ref[:, cols].astype(jnp.float32)
        sig = jax.nn.sigmoid(gate)
        gate_grad_ref[:, cols] = (grad * up_val * sig * (1.0 + gate * (1.0 - sig))).astype(jnp.bfloat16)
        up_grad_ref[:, cols] = (grad * gate * sig).astype(jnp.bfloat16)
        return carry

    lax.fori_loop(0, chunks // 2, input_step, 0)
    pass_on(back[-1])
    lax.fori_loop(chunks // 2, chunks, input_step, 0)

    part_copy.wait_recv()
    base = rep * half
    for g in range(half // group):
        some = weights[pl.ds(base + g * group, group)].reshape(group * rows, ff)
        own = lax.dot_general(
            hid[...], some, (((1,), (1,)), ((), ())), preferred_element_type=jnp.float32
        )
        out_ref[:, g * group * rows : (g + 1) * group * rows] = (own + part_recv[g]).astype(jnp.bfloat16)

    mid_wait(out)
    sources = [lax.rem(out + outer - k, outer) for k in range(1, outer)]
    for source in sources:
        remote(outer_recv.at[source], outer_recv.at[source], outer_send_sem.at[0], outer_recv_sem.at[source], mid_peer).wait_recv()

    loads[2].wait()
    loads[3].wait()

    def update_step(j, carry):
        cols = columns(j)
        grad = own_sum[out, :, cols] + mid_recv[out, :, cols].astype(jnp.float32)
        for source in sources:
            grad += outer_recv[source, :, cols].astype(jnp.float32)
        master_new, first, second = adam(
            grad / jnp.float32(total), master_ref[:, cols], one_ref[:, cols], two_ref[:, cols]
        )
        master_new_ref[:, cols] = master_new
        first_ref[:, cols] = first
        second_ref[:, cols] = second
        return carry

    lax.fori_loop(0, chunks, update_step, 0)
    for copy in started:
        copy.wait_send()


def handed_on(values):
    count = len(values)

    def body(*refs):
        sems = refs[-1]
        copies = [
            pltpu.make_async_copy(refs[index], refs[count + index], sems.at[index]) for index in range(count)
        ]
        for copy in copies:
            copy.start()
        for copy in copies:
            copy.wait()

    return pl.pallas_call(
        body,
        out_shape=[jax.ShapeDtypeStruct(value.shape, value.dtype) for value in values],
        in_specs=[pl.BlockSpec(memory_space=pltpu.VMEM)] * count,
        out_specs=[pl.BlockSpec(memory_space=pl.ANY)] * count,
        scratch_shapes=[pltpu.SemaphoreType.DMA((count,))],
        compiler_params=pltpu.CompilerParams(vmem_limit_bytes=8 * 1024 * 1024),
    )(*[pltpu.with_memory_space_constraint(value, pltpu.VMEM) for value in values])


def in_one_kernel(size, gate_pre, up_pre, out_grad, master, moment_one, moment_two):
    micro, count, ff = gate_pre.shape
    tokens, depth, rows = micro * count, out_grad.shape[2], master.shape[0]
    outer = size // (MID * CORES)
    half = size // 2
    group = max(1, min(half, 256 // rows))
    cot = out_grad.reshape(tokens, depth)
    vmem = pl.BlockSpec(memory_space=pltpu.VMEM)
    hbm = pl.BlockSpec(memory_space=pl.ANY)
    bf, f32 = jnp.bfloat16, jnp.float32
    dma = pltpu.SemaphoreType.DMA
    results = pl.pallas_call(
        functools.partial(fused, outer, tokens * size),
        out_shape=(
            pltpu.VMEM((tokens, depth // 2), bf),
            pltpu.VMEM((tokens, ff), bf),
            pltpu.VMEM((tokens, ff), bf),
            pltpu.VMEM((rows, ff), f32),
            pltpu.VMEM((rows, ff), f32),
            pltpu.VMEM((rows, ff), f32),
        ),
        in_specs=[hbm, hbm, vmem, vmem, hbm, hbm],
        out_specs=(vmem,) * 6,
        scratch_shapes=[
            pltpu.VMEM((size, rows, ff), bf),
            pltpu.VMEM((tokens, ff), bf),
            pltpu.VMEM((tokens, ff), bf),
            pltpu.VMEM((MID, outer, rows, tokens), bf),
            pltpu.VMEM((outer, rows, ff), f32),
            pltpu.VMEM((outer, rows, ff), bf),
            pltpu.VMEM((outer, rows, ff), bf),
            pltpu.VMEM((outer, rows, ff), bf),
            pltpu.VMEM((outer, rows, ff), bf),
            pltpu.VMEM((half // group, tokens, group * rows), f32),
            pltpu.VMEM((half // group, tokens, group * rows), f32),
            pltpu.VMEM((CORES, MID, outer, rows, tokens), bf),
            pltpu.VMEM((tokens, ff), bf),
            pltpu.VMEM((tokens, ff), bf),
            pltpu.VMEM((rows, ff), f32),
            pltpu.VMEM((rows, ff), f32),
            dma((4,)),
            dma((size,)), dma((outer,)), dma((outer,)), dma((2 * outer,)),
            dma((2,)), dma((2,)),
            dma((outer,)), dma((outer,)), dma((outer,)), dma((outer,)), dma, dma,
        ],
        compiler_params=pltpu.CompilerParams(
            collective_id=0, has_side_effects=True, vmem_limit_bytes=50 * 1024 * 1024
        ),
    )(
        gate_pre.reshape(tokens, ff), up_pre.reshape(tokens, ff), cot, master, moment_one, moment_two,
    )
    results = handed_on(results)
    split = [value.reshape(micro, count, value.shape[1]) for value in results[:3]]
    return (*split, *results[3:])


def with_collectives(gate_pre, up_pre, out_grad, master, moment_one, moment_two):
    weights = lax.all_gather(master.astype(jnp.bfloat16), "dp", axis=0, tiled=True)
    micro = gate_pre.shape[0]
    total = micro * gate_pre.shape[1] * lax.axis_size("dp")
    outs_list = []
    gate_list = []
    up_list = []
    grad_sum = None
    for index in range(micro):
        gate = gate_pre[index].astype(jnp.float32)
        up_val = up_pre[index].astype(jnp.float32)
        sig = jax.nn.sigmoid(gate)
        hidden = (gate * sig * up_val).astype(jnp.bfloat16)
        partial_out = lax.dot_general(
            hidden, weights, (((1,), (1,)), ((), ())), preferred_element_type=jnp.float32
        )
        outs_list.append(
            lax.psum_scatter(partial_out, "rep", scatter_dimension=1, tiled=True).astype(
                jnp.bfloat16
            )
        )
        hid_grad = jnp.dot(out_grad[index], weights, preferred_element_type=jnp.float32)
        gate_list.append(
            (hid_grad * up_val * sig * (1.0 + gate * (1.0 - sig))).astype(jnp.bfloat16)
        )
        up_list.append((hid_grad * gate * sig).astype(jnp.bfloat16))
        term = lax.dot_general(
            out_grad[index], hidden, (((0,), (0,)), ((), ())), preferred_element_type=jnp.float32
        )
        shard = lax.psum_scatter(term, "dp", scatter_dimension=0, tiled=True)
        grad_sum = shard if grad_sum is None else grad_sum + shard
    updated = adam(grad_sum / jnp.float32(total), master, moment_one, moment_two)
    return jnp.stack(outs_list), jnp.stack(gate_list), jnp.stack(up_list), *updated


def solution(mesh):
    size = mesh.shape["dp"]

    def on_device(gate_pre, up_pre, out_grad, master, moment_one, moment_two):
        tall = master.shape[0] % 16 == 0 and size % (MID * CORES) == 0 and size > MID * CORES
        step = functools.partial(in_one_kernel, size) if tall else with_collectives
        return step(gate_pre, up_pre, out_grad, master, moment_one, moment_two)

    split = P(None, "dp", "rep")
    owned = P("dp", "rep")
    return jax.shard_map(
        on_device,
        mesh=mesh,
        in_specs=(split, split, P(None, "dp", None), owned, owned, owned),
        out_specs=(split, split, split, owned, owned, owned),
        check_vma=False,
    )
```

```python
import functools

import jax
import jax.numpy as jnp
from jax import lax
from jax.experimental import pallas as pl
from jax.experimental.pallas import tpu as pltpu
from jax.sharding import PartitionSpec as P

first_power = 2.6561398887587544e-05
second_power = 0.005920529220333997

MESH = pl.DeviceIdType.MESH
CORES = 2
MID = 2
WIDTH = 256
ALONG = 0.32


def adam(main_grad, master, moment_one, moment_two):
    first = 0.9 * moment_one + 0.1 * main_grad
    second = 0.95 * moment_two + 0.05 * main_grad * main_grad
    update = first / (1.0 - first_power) / (jnp.sqrt(second / (1.0 - second_power)) + 1e-08)
    return master - 0.003 * (update + 0.1 * master), first, second


def fused(
    outer, total, split,
    gate_hbm, up_hbm, cot_hbm, master_hbm, one_hbm, two_hbm,
    out_ref, gate_grad_ref, up_grad_ref, master_new_ref, first_ref, second_ref,
    weights, hid, hid_peer, cot_peer, own_sum, mid_send, mid_recv, line_send, line_recv,
    part, part_send, part_recv, hid_grad, cot_rows_ref,
    gate_ref, up_ref, cot_ref, master_ref, one_ref, two_ref,
    local_sem, send_sem, w_recv, core_recv, mid_recv_sem, line_recv_sem, part_recv_sem,
):
    me = lax.axis_index("dp")
    rep = lax.axis_index("rep")
    core = lax.rem(me, CORES)
    mid = lax.rem(me // CORES, MID)
    out = me // (CORES * MID)
    n = outer * MID * CORES
    block = MID * CORES
    rows, ff = master_ref.shape
    tokens = gate_ref.shape[0]
    loads = [
        pltpu.make_async_copy(src, dst, local_sem.at[index])
        for index, (src, dst) in enumerate(
            (
                (master_hbm, master_ref), (gate_hbm, gate_ref), (up_hbm, up_ref), (cot_hbm, cot_ref),
                (one_hbm, one_ref), (two_hbm, two_ref),
            )
        )
    ]
    for load in loads:
        load.start()
    width = WIDTH
    chunks = ff // width
    lead = (chunks + 1) // 2
    pieces = (pl.ds(0, lead * width), pl.ds(lead * width, ff - lead * width))
    parts = (pl.ds(0, split), pl.ds(split, ff - split))
    last = outer - 1
    low = out < outer // 2

    def at(o, m, c):
        return (o * MID + m) * CORES + c

    core_peer = {"dp": at(out, mid, 1 - core)}
    mid_peer = {"dp": at(out, 1 - mid, core)}
    rep_peer = {"rep": 1 - rep}
    next_peer = {"dp": at(jnp.minimum(out + 1, last), mid, core)}
    prev_peer = {"dp": at(jnp.maximum(out - 1, 0), mid, core)}
    has_next = out < last
    has_prev = out > 0

    def remote(src, dst, send, recv, device):
        return pltpu.make_async_remote_copy(
            src_ref=src, dst_ref=dst, send_sem=send, recv_sem=recv,
            device_id=device, device_id_type=MESH,
        )

    started = []

    def go(ends, device, cond=None, inside=None):
        index = len(started)

        def make():
            src, dst, recv = ends()
            return remote(src, dst, send_sem.at[index], recv, device)

        if cond is None:
            make().start()
        else:
            pl.when(cond)(lambda: make().start())
        started.append((make, [given for given in (inside, cond) if given is not None]))

    barrier = pltpu.get_barrier_semaphore()
    for peer in (core_peer, mid_peer, rep_peer):
        pl.semaphore_signal(barrier, inc=1, device_id=peer, device_id_type=MESH)

    @pl.when(has_next)
    def _():
        pl.semaphore_signal(barrier, inc=1, device_id=next_peer, device_id_type=MESH)

    @pl.when(has_prev)
    def _():
        pl.semaphore_signal(barrier, inc=1, device_id=prev_peer, device_id_type=MESH)

    loads[0].wait()
    weights[me] = master_ref[...].astype(jnp.bfloat16)
    pl.semaphore_wait(barrier, 3 + has_next.astype(jnp.int32) + has_prev.astype(jnp.int32))

    def w_go(slot, which, device, cond=None, inside=None):
        def ends():
            ref = weights.at[slot, :, parts[which]]
            return ref, ref, w_recv.at[which, slot]

        go(ends, device, cond, inside)

    def w_wait(slot, which):
        ref = weights.at[slot, :, parts[which]]
        remote(ref, ref, send_sem.at[0], w_recv.at[which, slot], core_peer).wait_recv()

    w_go(me, 1, mid_peer)
    w_go(me, 0, next_peer, has_next)
    w_go(me, 0, prev_peer, has_prev)
    w_go(me, 1, next_peer, has_next)
    w_go(me, 1, prev_peer, has_prev)
    w_go(me, 0, mid_peer)
    w_go(me, 1, core_peer)
    w_go(me, 0, core_peer)

    def along(k, m, which):
        for cond, slot, device, more in (
            (out >= k, at(out - k, m, core), next_peer, has_next),
            (out + k <= last, at(out + k, m, core), prev_peer, has_prev),
        ):
            @pl.when(cond)
            def _():
                w_wait(slot, which)
                w_go(slot, which, device, more, cond)
                if which == 0:
                    w_go(slot, which, mid_peer, None, cond)
                w_go(slot, which, core_peer, None, cond)

    def across_first():
        slot = at(out, 1 - mid, core)
        w_wait(slot, 1)
        w_go(slot, 1, next_peer, has_next)
        w_go(slot, 1, prev_peer, has_prev)
        w_go(slot, 1, core_peer)

    def across_last(k):
        sides = ((out >= k, out - k), (out + k <= last, out + k))
        for cond, o in sides if k else sides[:1]:
            slot = at(o, 1 - mid, core)

            @pl.when(cond)
            def _():
                w_wait(slot, 0)
                w_go(slot, 0, core_peer, None, cond)

    loads[3].wait()
    turned = jnp.transpose(cot_ref[...].astype(jnp.float32)).astype(jnp.bfloat16).reshape(n, rows, tokens)
    for o in range(outer):
        for m in range(MID):
            for c in range(CORES):
                cot_rows_ref[c, m, o] = turned[at(o, m, c)]
    go(lambda: (cot_rows_ref.at[1 - core], cot_peer, core_recv.at[0]), core_peer)
    loads[1].wait()
    loads[2].wait()

    def columns(j):
        return pl.ds(pl.multiple_of(j * width, width), width)

    def hidden_step(j, carry):
        cols = columns(j)
        gate = gate_ref[:, cols].astype(jnp.float32)
        sig = jax.nn.sigmoid(gate)
        hid[:, cols] = (gate * sig * up_ref[:, cols].astype(jnp.float32)).astype(jnp.bfloat16)
        return carry

    bounds = ((0, lead), (lead, chunks))
    for p, (lo, hi) in enumerate(bounds):
        lax.fori_loop(lo, hi, hidden_step, 0)
        go(
            lambda p=p: (hid.at[:, pieces[p]], hid_peer.at[:, pieces[p]], core_recv.at[1 + p]),
            core_peer,
        )

    def core_wait(p):
        ref = hid_peer.at[:, pieces[p]]
        remote(ref, ref, send_sem.at[0], core_recv.at[1 + p], core_peer).wait_recv()

    def grad_of(which, cols):
        own = cot_rows_ref[core, which].reshape(outer * rows, tokens)
        other = cot_peer[which].reshape(outer * rows, tokens)
        value = jnp.dot(own, hid[:, cols], preferred_element_type=jnp.float32)
        value += jnp.dot(other, hid_peer[:, cols], preferred_element_type=jnp.float32)
        return value.reshape(outer, rows, width)

    def send_step(j, carry):
        cols = columns(j)
        mid_send[:, :, cols] = grad_of(1 - mid, cols).astype(jnp.bfloat16)
        return carry

    def own_step(j, carry):
        cols = columns(j)
        own_sum[:, :, cols] = grad_of(mid, cols)
        return carry

    def target(i):
        if i == last:
            return out
        down = last - i
        down = jnp.where(down <= out, down - 1, down)
        return jnp.where(low, down, jnp.where(i >= out, i + 1, i))

    def reduce_across(i):
        t = target(i)
        for h in range(2):
            go(
                lambda h=h: (
                    mid_send.at[t, :, pieces[h]], mid_recv.at[t, :, pieces[h]], mid_recv_sem.at[h, t],
                ),
                mid_peer,
            )

    def mid_wait(t, h):
        ref = mid_recv.at[t, :, pieces[h]]
        remote(ref, ref, send_sem.at[0], mid_recv_sem.at[h, t], mid_peer).wait_recv()

    def line_wait(d, t, h):
        ref = line_recv.at[d, t, :, pieces[h]]
        remote(ref, ref, send_sem.at[0], line_recv_sem.at[d, h, t], mid_peer).wait_recv()

    def pass_on(i, h, cond=None):
        t = target(i)
        d = jnp.where(t > out, 0, 1)
        more = jnp.where(t > out, has_prev, has_next)
        lo, hi = bounds[h]
        toward = {"dp": at(out + 1 - 2 * d, mid, core)}

        def step(chained):
            def inner(j, carry):
                cols = columns(j)
                value = own_sum[t, :, cols] + mid_recv[t, :, cols].astype(jnp.float32)
                if chained:
                    value += line_recv[d, t, :, cols].astype(jnp.float32)
                line_send[t, :, cols] = value.astype(jnp.bfloat16)
                return carry

            return inner

        def run():
            mid_wait(t, h)

            @pl.when(more)
            def _():
                line_wait(d, t, h)
                lax.fori_loop(lo, hi, step(True), 0)

            @pl.when(jnp.logical_not(more))
            def _():
                lax.fori_loop(lo, hi, step(False), 0)

            go(
                lambda: (
                    line_send.at[t, :, pieces[h]], line_recv.at[d, t, :, pieces[h]],
                    line_recv_sem.at[d, h, t],
                ),
                toward, None, cond,
            )

        if cond is None:
            run()
        else:
            pl.when(cond)(run)

    def nearest(j):
        if j == 0:
            return out
        k = (j + 1) // 2
        z = jnp.where(low, out, last - out)
        g = jnp.where(j <= 2 * z, z - k if j % 2 else z + k, j)
        return jnp.where(low, g, last - g)

    half = outer // 2
    deep = block * rows

    def use_block(j):
        g = nearest(j)
        for m in range(MID):
            for which in range(2):
                w_wait(at(g, m, 1 - core), which)
        some = weights[pl.ds(g * block, block)].reshape(deep, ff)
        value = lax.dot_general(hid[...], some, (((1,), (1,)), ((), ())), preferred_element_type=jnp.float32)
        part[g] = value
        part_send[g] = value.astype(jnp.bfloat16)
        place = lax.rem(g, half)
        go(
            lambda: (part_send.at[g], part_recv.at[place], part_recv_sem.at[place]),
            rep_peer, g // half != rep,
        )
        cot = cot_ref[:, pl.ds(pl.multiple_of(g * deep, deep), deep)]

        def step(i, carry):
            cols = columns(i)
            grad = jnp.dot(
                cot, weights[pl.ds(g * block, block), :, cols].reshape(deep, width),
                preferred_element_type=jnp.float32,
            )
            if j > 0:
                grad += hid_grad[:, cols]
            if j < last:
                hid_grad[:, cols] = grad
            else:
                gate = gate_ref[:, cols].astype(jnp.float32)
                up_val = up_ref[:, cols].astype(jnp.float32)
                sig = jax.nn.sigmoid(gate)
                gate_grad_ref[:, cols] = (grad * up_val * sig * (1.0 + gate * (1.0 - sig))).astype(jnp.bfloat16)
                up_grad_ref[:, cols] = (grad * gate * sig).astype(jnp.bfloat16)
            return carry

        lax.fori_loop(0, chunks, step, 0)

    edge = jnp.logical_or(out == 0, out == last)
    inner = jnp.logical_not(edge)
    along(1, mid, 0)
    for p, (lo, hi) in enumerate(bounds):
        if p == 0:
            ref = cot_peer
            remote(ref, ref, send_sem.at[0], core_recv.at[0], core_peer).wait_recv()
        core_wait(p)
        lax.fori_loop(lo, hi, send_step, 0)
        if p == 0:
            across_first()
    reduce_across(0)
    across_last(0)
    lax.fori_loop(0, chunks, own_step, 0)
    along(1, mid, 1)
    if outer > 2:
        along(2, mid, 0)
    reduce_across(1)
    use_block(0)
    across_last(1)
    along(1, 1 - mid, 1)
    pass_on(0, 0, edge)
    pass_on(0, 1, edge)
    use_block(1)
    for k in range(2, outer):
        across_last(k)
        if k == 2:
            pass_on(0, 0, inner)
        along(k, mid, 1)
        if k == 2:
            pass_on(0, 1, inner)
        if k < last:
            along(k + 1, mid, 0)
            reduce_across(k)
        if k == last - 1:
            reduce_across(last)
        pass_on(k - 1, 0)
        along(k, 1 - mid, 1)
        pass_on(k - 1, 1)
        use_block(k)
    loads[4].wait()
    loads[5].wait()

    @pl.when(jnp.logical_not(has_prev))
    def _():
        line_recv[0, out] = jnp.zeros((rows, ff), jnp.bfloat16)

    @pl.when(jnp.logical_not(has_next))
    def _():
        line_recv[1, out] = jnp.zeros((rows, ff), jnp.bfloat16)

    def update_step(j, carry):
        cols = columns(j)
        grad = own_sum[out, :, cols] + mid_recv[out, :, cols].astype(jnp.float32)
        grad += line_recv[0, out, :, cols].astype(jnp.float32) + line_recv[1, out, :, cols].astype(jnp.float32)
        master_new, first, second = adam(
            grad / jnp.float32(total), master_ref[:, cols], one_ref[:, cols], two_ref[:, cols]
        )
        master_new_ref[:, cols] = master_new
        first_ref[:, cols] = first
        second_ref[:, cols] = second
        return carry

    for h, (lo, hi) in enumerate(bounds):
        pl.when(has_prev)(lambda: line_wait(0, out, h))
        pl.when(has_next)(lambda: line_wait(1, out, h))
        mid_wait(out, h)
        lax.fori_loop(lo, hi, update_step, 0)

    for place in range(half):
        ref = part_recv.at[place]
        remote(ref, ref, send_sem.at[0], part_recv_sem.at[place], rep_peer).wait_recv()
        out_ref[:, place * deep : (place + 1) * deep] = (
            part[rep * half + place] + part_recv[place].astype(jnp.float32)
        ).astype(jnp.bfloat16)
    for make, given in started:
        if given:
            pl.when(functools.reduce(jnp.logical_and, given))(lambda: make().wait_send())
        else:
            make().wait_send()


def handed_on(values):
    count = len(values)

    def body(*refs):
        sems = refs[-1]
        copies = [
            pltpu.make_async_copy(refs[index], refs[count + index], sems.at[index]) for index in range(count)
        ]
        for copy in copies:
            copy.start()
        for copy in copies:
            copy.wait()

    return pl.pallas_call(
        body,
        out_shape=[jax.ShapeDtypeStruct(value.shape, value.dtype) for value in values],
        in_specs=[pl.BlockSpec(memory_space=pltpu.VMEM)] * count,
        out_specs=[pl.BlockSpec(memory_space=pl.ANY)] * count,
        scratch_shapes=[pltpu.SemaphoreType.DMA((count,))],
        compiler_params=pltpu.CompilerParams(vmem_limit_bytes=8 * 1024 * 1024),
    )(*[pltpu.with_memory_space_constraint(value, pltpu.VMEM) for value in values])


def in_one_kernel(size, gate_pre, up_pre, out_grad, master, moment_one, moment_two):
    micro, count, ff = gate_pre.shape
    tokens, depth, rows = micro * count, out_grad.shape[2], master.shape[0]
    outer = size // (MID * CORES)
    deep = MID * CORES * rows
    split = max(1, round(ff * ALONG / 128)) * 128
    cot = out_grad.reshape(tokens, depth)
    hbm = pl.BlockSpec(memory_space=pl.ANY)
    bf, f32 = jnp.bfloat16, jnp.float32
    dma = pltpu.SemaphoreType.DMA
    results = pl.pallas_call(
        functools.partial(fused, outer, tokens * size, split),
        out_shape=(
            pltpu.VMEM((tokens, depth // 2), bf),
            pltpu.VMEM((tokens, ff), bf),
            pltpu.VMEM((tokens, ff), bf),
            pltpu.VMEM((rows, ff), f32),
            pltpu.VMEM((rows, ff), f32),
            pltpu.VMEM((rows, ff), f32),
        ),
        in_specs=[hbm] * 6,
        out_specs=(pl.BlockSpec(memory_space=pltpu.VMEM),) * 6,
        scratch_shapes=[
            pltpu.VMEM((size, rows, ff), bf),
            pltpu.VMEM((tokens, ff), bf),
            pltpu.VMEM((tokens, ff), bf),
            pltpu.VMEM((MID, outer, rows, tokens), bf),
            pltpu.VMEM((outer, rows, ff), f32),
            pltpu.VMEM((outer, rows, ff), bf),
            pltpu.VMEM((outer, rows, ff), bf),
            pltpu.VMEM((outer, rows, ff), bf),
            pltpu.VMEM((2, outer, rows, ff), bf),
            pltpu.VMEM((outer, tokens, deep), f32),
            pltpu.VMEM((outer, tokens, deep), bf),
            pltpu.VMEM((outer // 2, tokens, deep), bf),
            pltpu.VMEM((tokens, ff), f32),
            pltpu.VMEM((CORES, MID, outer, rows, tokens), bf),
            pltpu.VMEM((tokens, ff), bf),
            pltpu.VMEM((tokens, ff), bf),
            pltpu.VMEM((tokens, depth), bf),
            pltpu.VMEM((rows, ff), f32),
            pltpu.VMEM((rows, ff), f32),
            pltpu.VMEM((rows, ff), f32),
            dma((6,)), dma((40 * outer,)), dma((2, size)), dma((3,)),
            dma((2, outer)), dma((2, 2, outer)), dma((outer // 2,)),
        ],
        compiler_params=pltpu.CompilerParams(
            collective_id=0, has_side_effects=True, vmem_limit_bytes=50 * 1024 * 1024
        ),
    )(
        gate_pre.reshape(tokens, ff), up_pre.reshape(tokens, ff), cot, master, moment_one, moment_two,
    )
    results = handed_on(results)
    split = [value.reshape(micro, count, value.shape[1]) for value in results[:3]]
    return (*split, *results[3:])


def with_collectives(gate_pre, up_pre, out_grad, master, moment_one, moment_two):
    weights = lax.all_gather(master.astype(jnp.bfloat16), "dp", axis=0, tiled=True)
    micro = gate_pre.shape[0]
    total = micro * gate_pre.shape[1] * lax.axis_size("dp")
    outs_list = []
    gate_list = []
    up_list = []
    grad_sum = None
    for index in range(micro):
        gate = gate_pre[index].astype(jnp.float32)
        up_val = up_pre[index].astype(jnp.float32)
        sig = jax.nn.sigmoid(gate)
        hidden = (gate * sig * up_val).astype(jnp.bfloat16)
        partial_out = lax.dot_general(
            hidden, weights, (((1,), (1,)), ((), ())), preferred_element_type=jnp.float32
        )
        outs_list.append(
            lax.psum_scatter(partial_out, "rep", scatter_dimension=1, tiled=True).astype(
                jnp.bfloat16
            )
        )
        hid_grad = jnp.dot(out_grad[index], weights, preferred_element_type=jnp.float32)
        gate_list.append(
            (hid_grad * up_val * sig * (1.0 + gate * (1.0 - sig))).astype(jnp.bfloat16)
        )
        up_list.append((hid_grad * gate * sig).astype(jnp.bfloat16))
        term = lax.dot_general(
            out_grad[index], hidden, (((0,), (0,)), ((), ())), preferred_element_type=jnp.float32
        )
        shard = lax.psum_scatter(term, "dp", scatter_dimension=0, tiled=True)
        grad_sum = shard if grad_sum is None else grad_sum + shard
    updated = adam(grad_sum / jnp.float32(total), master, moment_one, moment_two)
    return jnp.stack(outs_list), jnp.stack(gate_list), jnp.stack(up_list), *updated


def solution(mesh):
    size = mesh.shape["dp"]

    def on_device(gate_pre, up_pre, out_grad, master, moment_one, moment_two):
        tall = master.shape[0] % 32 == 0 and master.shape[1] % WIDTH == 0 and size % (2 * MID * CORES) == 0
        step = functools.partial(in_one_kernel, size) if tall else with_collectives
        return step(gate_pre, up_pre, out_grad, master, moment_one, moment_two)

    split = P(None, "dp", "rep")
    owned = P("dp", "rep")
    return jax.shard_map(
        on_device,
        mesh=mesh,
        in_specs=(split, split, P(None, "dp", None), owned, owned, owned),
        out_specs=(split, split, split, owned, owned, owned),
        check_vma=False,
    )
```

```python
import functools

import jax
import jax.numpy as jnp
from jax import lax
from jax.experimental import pallas as pl
from jax.experimental.pallas import tpu as pltpu
from jax.sharding import PartitionSpec as P

first_power = 2.6561398887587544e-05
second_power = 0.005920529220333997

MESH = pl.DeviceIdType.MESH
CORES = 2
MID = 2
WIDTH = 256
ALONG = 0.6
ACROSS = 0.636


def adam(main_grad, master, moment_one, moment_two):
    first = 0.9 * moment_one + 0.1 * main_grad
    second = 0.95 * moment_two + 0.05 * main_grad * main_grad
    update = first / (1.0 - first_power) / (jnp.sqrt(second / (1.0 - second_power)) + 1e-08)
    return master - 0.003 * (update + 0.1 * master), first, second


def fused(
    outer, total, split, early,
    gate_hbm, up_hbm, cot_hbm, master_hbm, one_hbm, two_hbm,
    out_ref, gate_grad_ref, up_grad_ref, master_new_ref, first_ref, second_ref,
    weights, hid, hid_peer, cot_peer, own_sum, mid_send, mid_recv, line_send, line_recv,
    wide_sum, wide_send, wide_recv, cross_send, cross_recv,
    part, part_send, part_recv, hid_grad, cot_rows_ref,
    gate_ref, up_ref, cot_ref, master_ref, one_ref, two_ref,
    local_sem, send_sem, w_recv, core_recv, mid_recv_sem, line_recv_sem, wide_recv_sem, cross_recv_sem, part_recv_sem,
):
    me = lax.axis_index("dp")
    rep = lax.axis_index("rep")
    core = lax.rem(me, CORES)
    mid = lax.rem(me // CORES, MID)
    out = me // (CORES * MID)
    n = outer * MID * CORES
    block = MID * CORES
    rows, ff = master_ref.shape
    tokens = gate_ref.shape[0]
    loads = [
        pltpu.make_async_copy(src, dst, local_sem.at[index])
        for index, (src, dst) in enumerate(
            (
                (master_hbm, master_ref), (gate_hbm, gate_ref), (up_hbm, up_ref), (cot_hbm, cot_ref),
                (one_hbm, one_ref), (two_hbm, two_ref),
            )
        )
    ]
    for load in loads:
        load.start()
    width = WIDTH
    chunks = ff // width
    first = early // width
    lead = (first + 1) // 2
    bounds = ((0, lead), (lead, first))
    pieces = (pl.ds(0, lead * width), pl.ds(lead * width, early - lead * width))
    sides = ((first, chunks), (0, first))
    halves = (pl.ds(early, ff - early), pl.ds(0, early))
    parts = (pl.ds(0, split), pl.ds(split, ff - split))
    last = outer - 1
    low = out < outer // 2

    def at(o, m, c):
        return (o * MID + m) * CORES + c

    core_peer = {"dp": at(out, mid, 1 - core)}
    mid_peer = {"dp": at(out, 1 - mid, core)}
    rep_peer = {"rep": 1 - rep}
    next_peer = {"dp": at(jnp.minimum(out + 1, last), mid, core)}
    prev_peer = {"dp": at(jnp.maximum(out - 1, 0), mid, core)}
    has_next = out < last
    has_prev = out > 0

    def remote(src, dst, send, recv, device):
        return pltpu.make_async_remote_copy(
            src_ref=src, dst_ref=dst, send_sem=send, recv_sem=recv,
            device_id=device, device_id_type=MESH,
        )

    started = []

    def go(ends, device, cond=None, inside=None):
        index = len(started)

        def make():
            src, dst, recv = ends()
            return remote(src, dst, send_sem.at[index], recv, device)

        if cond is None:
            make().start()
        else:
            pl.when(cond)(lambda: make().start())
        started.append((make, [given for given in (inside, cond) if given is not None]))

    barrier = pltpu.get_barrier_semaphore()
    for peer in (core_peer, mid_peer, rep_peer):
        pl.semaphore_signal(barrier, inc=1, device_id=peer, device_id_type=MESH)

    @pl.when(has_next)
    def _():
        pl.semaphore_signal(barrier, inc=1, device_id=next_peer, device_id_type=MESH)

    @pl.when(has_prev)
    def _():
        pl.semaphore_signal(barrier, inc=1, device_id=prev_peer, device_id_type=MESH)

    loads[0].wait()
    weights[me] = master_ref[...].astype(jnp.bfloat16)
    pl.semaphore_wait(barrier, 3 + has_next.astype(jnp.int32) + has_prev.astype(jnp.int32))

    def w_go(slot, which, device, cond=None, inside=None):
        def ends():
            ref = weights.at[slot, :, parts[which]]
            return ref, ref, w_recv.at[which, slot]

        go(ends, device, cond, inside)

    def w_wait(slot, which):
        ref = weights.at[slot, :, parts[which]]
        remote(ref, ref, send_sem.at[0], w_recv.at[which, slot], core_peer).wait_recv()

    w_go(me, 1, mid_peer)
    w_go(me, 0, next_peer, has_next)
    w_go(me, 0, prev_peer, has_prev)
    w_go(me, 1, next_peer, has_next)
    w_go(me, 1, prev_peer, has_prev)
    w_go(me, 0, mid_peer)
    w_go(me, 1, core_peer)
    w_go(me, 0, core_peer)

    def along(k, m, which):
        for cond, slot, device, more in (
            (out >= k, at(out - k, m, core), next_peer, has_next),
            (out + k <= last, at(out + k, m, core), prev_peer, has_prev),
        ):
            @pl.when(cond)
            def _():
                w_wait(slot, which)
                w_go(slot, which, device, more, cond)
                if which == 0:
                    w_go(slot, which, mid_peer, None, cond)
                w_go(slot, which, core_peer, None, cond)

    def across_first():
        slot = at(out, 1 - mid, core)
        w_wait(slot, 1)
        w_go(slot, 1, next_peer, has_next)
        w_go(slot, 1, prev_peer, has_prev)
        w_go(slot, 1, core_peer)

    def across_last(k):
        sides = ((out >= k, out - k), (out + k <= last, out + k))
        for cond, o in sides if k else sides[:1]:
            slot = at(o, 1 - mid, core)

            @pl.when(cond)
            def _():
                w_wait(slot, 0)
                w_go(slot, 0, core_peer, None, cond)

    loads[3].wait()
    turned = jnp.transpose(cot_ref[...].astype(jnp.float32)).astype(jnp.bfloat16).reshape(n, rows, tokens)
    for o in range(outer):
        for m in range(MID):
            for c in range(CORES):
                cot_rows_ref[c, m, o] = turned[at(o, m, c)]
    go(lambda: (cot_rows_ref.at[1 - core], cot_peer, core_recv.at[0]), core_peer)
    loads[1].wait()
    loads[2].wait()

    def columns(j):
        return pl.ds(pl.multiple_of(j * width, width), width)

    def hidden_step(j, carry):
        cols = columns(j)
        gate = gate_ref[:, cols].astype(jnp.float32)
        sig = jax.nn.sigmoid(gate)
        hid[:, cols] = (gate * sig * up_ref[:, cols].astype(jnp.float32)).astype(jnp.bfloat16)
        return carry

    for p, (lo, hi) in enumerate(sides):
        lax.fori_loop(lo, hi, hidden_step, 0)
        go(
            lambda p=p: (hid.at[:, halves[p]], hid_peer.at[:, halves[p]], core_recv.at[1 + p]),
            core_peer,
        )

    def core_wait(p):
        ref = hid_peer.at[:, halves[p]]
        remote(ref, ref, send_sem.at[0], core_recv.at[1 + p], core_peer).wait_recv()

    def grad_of(which, cols):
        own = cot_rows_ref[core, which].reshape(outer * rows, tokens)
        other = cot_peer[which].reshape(outer * rows, tokens)
        value = jnp.dot(own, hid[:, cols], preferred_element_type=jnp.float32)
        value += jnp.dot(other, hid_peer[:, cols], preferred_element_type=jnp.float32)
        return value.reshape(outer, rows, width)

    def send_step(j, carry):
        cols = columns(j)
        mid_send[:, :, cols] = grad_of(1 - mid, cols).astype(jnp.bfloat16)
        return carry

    def wide_columns(j):
        return pl.ds(pl.multiple_of(j * width - early, width), width)

    def wide_step(j, carry):
        for m in range(MID):
            wide_sum[m, :, :, wide_columns(j)] = grad_of(m, columns(j))
        return carry

    def own_step(j, carry):
        cols = columns(j)
        own_sum[:, :, cols] = grad_of(mid, cols)
        return carry

    def target(i):
        if i == last:
            return out
        down = last - i
        down = jnp.where(down <= out, down - 1, down)
        return jnp.where(low, down, jnp.where(i >= out, i + 1, i))

    def reduce_across(i):
        t = target(i)
        for h in range(2):
            go(
                lambda h=h: (
                    mid_send.at[t, :, pieces[h]], mid_recv.at[t, :, pieces[h]], mid_recv_sem.at[h, t],
                ),
                mid_peer,
            )

    def mid_wait(t, h):
        ref = mid_recv.at[t, :, pieces[h]]
        remote(ref, ref, send_sem.at[0], mid_recv_sem.at[h, t], mid_peer).wait_recv()

    def line_wait(d, t, h):
        ref = line_recv.at[d, t, :, pieces[h]]
        remote(ref, ref, send_sem.at[0], line_recv_sem.at[d, h, t], mid_peer).wait_recv()

    def pass_on(i, h, cond=None):
        t = target(i)
        d = jnp.where(t > out, 0, 1)
        more = jnp.where(t > out, has_prev, has_next)
        lo, hi = bounds[h]
        toward = {"dp": at(out + 1 - 2 * d, mid, core)}

        def step(chained):
            def inner(j, carry):
                cols = columns(j)
                value = own_sum[t, :, cols] + mid_recv[t, :, cols].astype(jnp.float32)
                if chained:
                    value += line_recv[d, t, :, cols].astype(jnp.float32)
                line_send[t, :, cols] = value.astype(jnp.bfloat16)
                return carry

            return inner

        def run():
            mid_wait(t, h)

            @pl.when(more)
            def _():
                line_wait(d, t, h)
                lax.fori_loop(lo, hi, step(True), 0)

            @pl.when(jnp.logical_not(more))
            def _():
                lax.fori_loop(lo, hi, step(False), 0)

            go(
                lambda: (
                    line_send.at[t, :, pieces[h]], line_recv.at[d, t, :, pieces[h]],
                    line_recv_sem.at[d, h, t],
                ),
                toward, None, cond,
            )

        if cond is None:
            run()
        else:
            pl.when(cond)(run)

    def wide_wait(d, m, t):
        ref = wide_recv.at[d, m, t]
        remote(ref, ref, send_sem.at[0], wide_recv_sem.at[d, m, t], mid_peer).wait_recv()

    def wide_on(i, p, cond=None):
        t = target(i)
        m = mid if p else 1 - mid
        d = jnp.where(t > out, 0, 1)
        more = jnp.where(t > out, has_prev, has_next)
        toward = {"dp": at(out + 1 - 2 * d, mid, core)}

        def step(chained):
            def inner(j, carry):
                cols = wide_columns(j)
                value = wide_sum[m, t, :, cols]
                if chained:
                    value += wide_recv[d, m, t, :, cols].astype(jnp.float32)
                wide_send[m, t, :, cols] = value.astype(jnp.bfloat16)
                return carry

            return inner

        def run():
            @pl.when(more)
            def _():
                wide_wait(d, m, t)
                lax.fori_loop(first, chunks, step(True), 0)

            @pl.when(jnp.logical_not(more))
            def _():
                lax.fori_loop(first, chunks, step(False), 0)

            go(
                lambda: (wide_send.at[m, t], wide_recv.at[d, m, t], wide_recv_sem.at[d, m, t]),
                toward, None, cond,
            )

        if cond is None:
            run()
        else:
            pl.when(cond)(run)

    def wide_total(m, cols):
        value = wide_sum[m, out, :, cols]
        value += wide_recv[0, m, out, :, cols].astype(jnp.float32)
        return value + wide_recv[1, m, out, :, cols].astype(jnp.float32)

    def wide_arrived(m):
        pl.when(has_prev)(lambda: wide_wait(0, m, out))
        pl.when(has_next)(lambda: wide_wait(1, m, out))

    def wide_across():
        wide_arrived(1 - mid)

        def step(j, carry):
            cols = wide_columns(j)
            cross_send[:, cols] = wide_total(1 - mid, cols).astype(jnp.bfloat16)
            return carry

        lax.fori_loop(first, chunks, step, 0)
        go(lambda: (cross_send, cross_recv, cross_recv_sem), mid_peer)

    @pl.when(jnp.logical_not(has_prev))
    def _():
        line_recv[0, out] = jnp.zeros((rows, early), jnp.bfloat16)
        wide_recv[0, :, out] = jnp.zeros((MID, rows, ff - early), jnp.bfloat16)

    @pl.when(jnp.logical_not(has_next))
    def _():
        line_recv[1, out] = jnp.zeros((rows, early), jnp.bfloat16)
        wide_recv[1, :, out] = jnp.zeros((MID, rows, ff - early), jnp.bfloat16)

    def nearest(j):
        if j == 0:
            return out
        k = (j + 1) // 2
        z = jnp.where(low, out, last - out)
        g = jnp.where(j <= 2 * z, z - k if j % 2 else z + k, j)
        return jnp.where(low, g, last - g)

    half = outer // 2
    deep = block * rows

    def use_block(j):
        g = nearest(j)
        for m in range(MID):
            for which in range(2):
                w_wait(at(g, m, 1 - core), which)
        some = weights[pl.ds(g * block, block)].reshape(deep, ff)
        value = lax.dot_general(hid[...], some, (((1,), (1,)), ((), ())), preferred_element_type=jnp.float32)
        part[g] = value
        part_send[g] = value.astype(jnp.bfloat16)
        place = lax.rem(g, half)
        go(
            lambda: (part_send.at[g], part_recv.at[place], part_recv_sem.at[place]),
            rep_peer, g // half != rep,
        )
        cot = cot_ref[:, pl.ds(pl.multiple_of(g * deep, deep), deep)]

        def step(i, carry):
            cols = columns(i)
            grad = jnp.dot(
                cot, weights[pl.ds(g * block, block), :, cols].reshape(deep, width),
                preferred_element_type=jnp.float32,
            )
            if j > 0:
                grad += hid_grad[:, cols]
            if j < last:
                hid_grad[:, cols] = grad
            else:
                gate = gate_ref[:, cols].astype(jnp.float32)
                up_val = up_ref[:, cols].astype(jnp.float32)
                sig = jax.nn.sigmoid(gate)
                gate_grad_ref[:, cols] = (grad * up_val * sig * (1.0 + gate * (1.0 - sig))).astype(jnp.bfloat16)
                up_grad_ref[:, cols] = (grad * gate * sig).astype(jnp.bfloat16)
            return carry

        lax.fori_loop(0, chunks, step, 0)

    edge = jnp.logical_or(out == 0, out == last)
    inner = jnp.logical_not(edge)
    ref = cot_peer
    remote(ref, ref, send_sem.at[0], core_recv.at[0], core_peer).wait_recv()
    core_wait(0)
    lax.fori_loop(first, chunks, wide_step, 0)
    for p in range(MID):
        wide_on(0, p, edge)
    across_first()
    along(1, mid, 0)
    core_wait(1)
    lax.fori_loop(0, first, send_step, 0)
    reduce_across(0)
    lax.fori_loop(0, first, own_step, 0)
    along(1, mid, 1)
    if last > 1:
        for p in range(MID):
            wide_on(1, p, edge)
    across_last(0)
    along(1, 1 - mid, 1)
    use_block(0)
    across_last(1)
    wide_on(0, 0, inner)
    pass_on(0, 0, edge)
    if last > 1:
        along(2, mid, 0)
    reduce_across(1)
    wide_on(0, 1, inner)
    pass_on(0, 1, edge)
    if last > 1:
        use_block(1)
    for k in range(2, outer):
        along(k, mid, 1)
        if k == 2:
            wide_on(1, 0, inner)
        along(k, 1 - mid, 1)
        if k == 2:
            wide_on(1, 1, inner)
        if k < last:
            for p in range(MID):
                wide_on(k, p, edge)
        if k == 2:
            pass_on(0, 0, inner)
        if k < last:
            along(k + 1, mid, 0)
            reduce_across(k)
        if k == last - 1:
            reduce_across(last)
        if k == 2:
            pass_on(0, 1, inner)
        if k < last:
            for p in range(MID):
                wide_on(k, p, inner)
        across_last(k)
        if k < last:
            pass_on(k - 1, 0, edge)
            pass_on(k - 1, 1, edge)
            use_block(k)
    for h in range(2):
        for k in range(last - 1, 0, -1):
            pass_on(k, h, inner)
    wide_across()
    if last > 1:
        pass_on(last - 1, 0, edge)
        pass_on(last - 1, 1, edge)
    use_block(last)
    loads[4].wait()
    loads[5].wait()

    def update_step(total_of):
        def step(j, carry):
            cols = columns(j)
            master_new, moment, square = adam(
                total_of(j) / jnp.float32(total), master_ref[:, cols], one_ref[:, cols], two_ref[:, cols]
            )
            master_new_ref[:, cols] = master_new
            first_ref[:, cols] = moment
            second_ref[:, cols] = square
            return carry

        return step

    def early_total(j):
        cols = columns(j)
        value = own_sum[out, :, cols] + mid_recv[out, :, cols].astype(jnp.float32)
        return value + line_recv[0, out, :, cols].astype(jnp.float32) + line_recv[1, out, :, cols].astype(jnp.float32)

    def late_total(j):
        cols = wide_columns(j)
        return wide_total(mid, cols) + cross_recv[:, cols].astype(jnp.float32)

    for h, (lo, hi) in enumerate(bounds):
        pl.when(has_prev)(lambda: line_wait(0, out, h))
        pl.when(has_next)(lambda: line_wait(1, out, h))
        mid_wait(out, h)
        lax.fori_loop(lo, hi, update_step(early_total), 0)
    wide_arrived(mid)
    remote(cross_recv, cross_recv, send_sem.at[0], cross_recv_sem, mid_peer).wait_recv()
    lax.fori_loop(first, chunks, update_step(late_total), 0)

    for place in range(half):
        ref = part_recv.at[place]
        remote(ref, ref, send_sem.at[0], part_recv_sem.at[place], rep_peer).wait_recv()
        out_ref[:, place * deep : (place + 1) * deep] = (
            part[rep * half + place] + part_recv[place].astype(jnp.float32)
        ).astype(jnp.bfloat16)
    for make, given in started:
        if given:
            pl.when(functools.reduce(jnp.logical_and, given))(lambda: make().wait_send())
        else:
            make().wait_send()


def handed_on(values):
    count = len(values)

    def body(*refs):
        sems = refs[-1]
        copies = [
            pltpu.make_async_copy(refs[index], refs[count + index], sems.at[index]) for index in range(count)
        ]
        for copy in copies:
            copy.start()
        for copy in copies:
            copy.wait()

    return pl.pallas_call(
        body,
        out_shape=[jax.ShapeDtypeStruct(value.shape, value.dtype) for value in values],
        in_specs=[pl.BlockSpec(memory_space=pltpu.VMEM)] * count,
        out_specs=[pl.BlockSpec(memory_space=pl.ANY)] * count,
        scratch_shapes=[pltpu.SemaphoreType.DMA((count,))],
        compiler_params=pltpu.CompilerParams(vmem_limit_bytes=8 * 1024 * 1024),
    )(*[pltpu.with_memory_space_constraint(value, pltpu.VMEM) for value in values])


def in_one_kernel(size, gate_pre, up_pre, out_grad, master, moment_one, moment_two):
    micro, count, ff = gate_pre.shape
    tokens, depth, rows = micro * count, out_grad.shape[2], master.shape[0]
    outer = size // (MID * CORES)
    deep = MID * CORES * rows
    split = max(1, round(ff * ALONG / 128)) * 128
    early = max(1, round(ff * ACROSS / WIDTH)) * WIDTH
    cot = out_grad.reshape(tokens, depth)
    hbm = pl.BlockSpec(memory_space=pl.ANY)
    bf, f32 = jnp.bfloat16, jnp.float32
    dma = pltpu.SemaphoreType.DMA
    results = pl.pallas_call(
        functools.partial(fused, outer, tokens * size, split, early),
        out_shape=(
            pltpu.VMEM((tokens, depth // 2), bf),
            pltpu.VMEM((tokens, ff), bf),
            pltpu.VMEM((tokens, ff), bf),
            pltpu.VMEM((rows, ff), f32),
            pltpu.VMEM((rows, ff), f32),
            pltpu.VMEM((rows, ff), f32),
        ),
        in_specs=[hbm] * 6,
        out_specs=(pl.BlockSpec(memory_space=pltpu.VMEM),) * 6,
        scratch_shapes=[
            pltpu.VMEM((size, rows, ff), bf),
            pltpu.VMEM((tokens, ff), bf),
            pltpu.VMEM((tokens, ff), bf),
            pltpu.VMEM((MID, outer, rows, tokens), bf),
            pltpu.VMEM((outer, rows, early), f32),
            pltpu.VMEM((outer, rows, early), bf),
            pltpu.VMEM((outer, rows, early), bf),
            pltpu.VMEM((outer, rows, early), bf),
            pltpu.VMEM((2, outer, rows, early), bf),
            pltpu.VMEM((MID, outer, rows, ff - early), f32),
            pltpu.VMEM((MID, outer, rows, ff - early), bf),
            pltpu.VMEM((2, MID, outer, rows, ff - early), bf),
            pltpu.VMEM((rows, ff - early), bf),
            pltpu.VMEM((rows, ff - early), bf),
            pltpu.VMEM((outer, tokens, deep), f32),
            pltpu.VMEM((outer, tokens, deep), bf),
            pltpu.VMEM((outer // 2, tokens, deep), bf),
            pltpu.VMEM((tokens, ff), f32),
            pltpu.VMEM((CORES, MID, outer, rows, tokens), bf),
            pltpu.VMEM((tokens, ff), bf),
            pltpu.VMEM((tokens, ff), bf),
            pltpu.VMEM((tokens, depth), bf),
            pltpu.VMEM((rows, ff), f32),
            pltpu.VMEM((rows, ff), f32),
            pltpu.VMEM((rows, ff), f32),
            dma((6,)), dma((40 * outer,)), dma((2, size)), dma((3,)),
            dma((2, outer)), dma((2, 2, outer)), dma((2, MID, outer)), dma, dma((outer // 2,)),
        ],
        compiler_params=pltpu.CompilerParams(
            collective_id=0, has_side_effects=True, vmem_limit_bytes=50 * 1024 * 1024
        ),
    )(
        gate_pre.reshape(tokens, ff), up_pre.reshape(tokens, ff), cot, master, moment_one, moment_two,
    )
    results = handed_on(results)
    split = [value.reshape(micro, count, value.shape[1]) for value in results[:3]]
    return (*split, *results[3:])


def with_collectives(gate_pre, up_pre, out_grad, master, moment_one, moment_two):
    weights = lax.all_gather(master.astype(jnp.bfloat16), "dp", axis=0, tiled=True)
    micro = gate_pre.shape[0]
    total = micro * gate_pre.shape[1] * lax.axis_size("dp")
    outs_list = []
    gate_list = []
    up_list = []
    grad_sum = None
    for index in range(micro):
        gate = gate_pre[index].astype(jnp.float32)
        up_val = up_pre[index].astype(jnp.float32)
        sig = jax.nn.sigmoid(gate)
        hidden = (gate * sig * up_val).astype(jnp.bfloat16)
        partial_out = lax.dot_general(
            hidden, weights, (((1,), (1,)), ((), ())), preferred_element_type=jnp.float32
        )
        outs_list.append(
            lax.psum_scatter(partial_out, "rep", scatter_dimension=1, tiled=True).astype(
                jnp.bfloat16
            )
        )
        hid_grad = jnp.dot(out_grad[index], weights, preferred_element_type=jnp.float32)
        gate_list.append(
            (hid_grad * up_val * sig * (1.0 + gate * (1.0 - sig))).astype(jnp.bfloat16)
        )
        up_list.append((hid_grad * gate * sig).astype(jnp.bfloat16))
        term = lax.dot_general(
            out_grad[index], hidden, (((0,), (0,)), ((), ())), preferred_element_type=jnp.float32
        )
        shard = lax.psum_scatter(term, "dp", scatter_dimension=0, tiled=True)
        grad_sum = shard if grad_sum is None else grad_sum + shard
    updated = adam(grad_sum / jnp.float32(total), master, moment_one, moment_two)
    return jnp.stack(outs_list), jnp.stack(gate_list), jnp.stack(up_list), *updated


def solution(mesh):
    size = mesh.shape["dp"]

    def on_device(gate_pre, up_pre, out_grad, master, moment_one, moment_two):
        tall = master.shape[0] % 32 == 0 and master.shape[1] % WIDTH == 0 and size in (2 * MID * CORES, 4 * MID * CORES)
        step = functools.partial(in_one_kernel, size) if tall else with_collectives
        return step(gate_pre, up_pre, out_grad, master, moment_one, moment_two)

    split = P(None, "dp", "rep")
    owned = P("dp", "rep")
    return jax.shard_map(
        on_device,
        mesh=mesh,
        in_specs=(split, split, P(None, "dp", None), owned, owned, owned),
        out_specs=(split, split, split, owned, owned, owned),
        check_vma=False,
    )
```

```python
import functools

import jax
import jax.numpy as jnp
from jax import lax
from jax.experimental import pallas as pl
from jax.experimental.pallas import tpu as pltpu
from jax.sharding import PartitionSpec as P

first_power = 2.6561398887587544e-05
second_power = 0.005920529220333997

MESH = pl.DeviceIdType.MESH
CORES = 2
MID = 2
LINE = 4
LANES = 128
WIDTH = 256
BROAD = 1408
ALONG = 0.591
ACROSS = 0.591
LEAD = 0.462
ORDER = (
    ("first",), ("core", 0), ("core", 1), ("along", 1, 0, 0), ("wide",), ("wedge", 0, 0), ("send",),
    ("across", 1, 0), ("wedge", 0, 1), ("last", 0), ("across", 0, 0), ("block", 0), ("along", 1, 0, 1),
    ("across", 0, 1), ("across", 1, 1), ("wedge", 1, 0), ("winner", 0, 0), ("wedge", 2, 0),
    ("along", 1, 1, 1), ("own",), ("along", 2, 0, 0), ("edge", 0, 1), ("winner", 0, 1), ("edge", 1, 1),
    ("winner", 2, 0), ("across", 2, 1), ("edge", 0, 0), ("last", 1), ("wedge", 1, 1), ("winner", 1, 0),
    ("inner", 0, 1), ("across", 2, 0), ("along", 2, 0, 1), ("edge", 1, 0), ("block", 1), ("along", 2, 1, 1),
    ("wedge", 2, 1), ("along", 3, 0, 0), ("across", 3, 1), ("inner", 1, 1), ("winner", 2, 1), ("last", 2),
    ("inner", 0, 0), ("edge", 2, 1), ("cross",), ("block", 2), ("edge", 2, 0), ("across", 3, 0),
    ("along", 3, 0, 1), ("along", 3, 1, 1), ("last", 3), ("winner", 1, 1), ("inner", 2, 1), ("block", 3),
    ("inner", 2, 0), ("inner", 1, 0), ("fin", 1), ("finw",), ("fin", 0),
)


def adam(main_grad, master, moment_one, moment_two):
    first = 0.9 * moment_one + 0.1 * main_grad
    second = 0.95 * moment_two + 0.05 * main_grad * main_grad
    update = first / (1.0 - first_power) / (jnp.sqrt(second / (1.0 - second_power)) + 1e-08)
    return master - 0.003 * (update + 0.1 * master), first, second


def fused(
    outer, total, split, early,
    gate_hbm, up_hbm, cot_hbm, master_hbm, one_hbm, two_hbm,
    out_ref, gate_grad_ref, up_grad_ref, master_new_ref, first_ref, second_ref,
    weights, hid, hid_peer, cot_peer, own_sum, mid_send, mid_recv, line_send, line_recv,
    wide_sum, wide_send, wide_recv, cross_send, cross_recv,
    part, part_send, part_recv, hid_grad, cot_rows_ref,
    gate_ref, up_ref, cot_ref, master_ref, one_ref, two_ref,
    local_sem, send_sem, w_recv, core_recv, mid_recv_sem, line_recv_sem, wide_recv_sem, cross_recv_sem, part_recv_sem,
):
    me = lax.axis_index("dp")
    rep = lax.axis_index("rep")
    core = lax.rem(me, CORES)
    mid = lax.rem(me // CORES, MID)
    out = me // (CORES * MID)
    n = outer * MID * CORES
    block = MID * CORES
    rows, ff = master_ref.shape
    tokens = gate_ref.shape[0]
    lead = max(1, round(early * LEAD / LANES)) * LANES
    bounds = ((0, lead), (lead, early))
    pieces = tuple(pl.ds(lo, hi - lo) for lo, hi in bounds)
    sides = ((early, ff), (0, early))
    halves = tuple(pl.ds(lo, hi - lo) for lo, hi in sides)
    parts = (pl.ds(0, split), pl.ds(split, ff - split))
    last = outer - 1
    low = out < outer // 2

    def at(o, m, c):
        return (o * MID + m) * CORES + c

    core_peer = {"dp": at(out, mid, 1 - core)}
    mid_peer = {"dp": at(out, 1 - mid, core)}
    rep_peer = {"rep": 1 - rep}
    next_peer = {"dp": at(jnp.minimum(out + 1, last), mid, core)}
    prev_peer = {"dp": at(jnp.maximum(out - 1, 0), mid, core)}
    has_next = out < last
    has_prev = out > 0

    def remote(src, dst, send, recv, device):
        return pltpu.make_async_remote_copy(
            src_ref=src, dst_ref=dst, send_sem=send, recv_sem=recv,
            device_id=device, device_id_type=MESH,
        )

    started = []

    def go(ends, device, cond=None, inside=None):
        index = len(started)

        def make():
            src, dst, recv = ends()
            return remote(src, dst, send_sem.at[index], recv, device)

        if cond is None:
            make().start()
        else:
            pl.when(cond)(lambda: make().start())
        started.append((make, [given for given in (inside, cond) if given is not None]))

    barrier = pltpu.get_barrier_semaphore()
    for peer in (core_peer, mid_peer, rep_peer):
        pl.semaphore_signal(barrier, inc=1, device_id=peer, device_id_type=MESH)

    @pl.when(has_next)
    def _():
        pl.semaphore_signal(barrier, inc=1, device_id=next_peer, device_id_type=MESH)

    @pl.when(has_prev)
    def _():
        pl.semaphore_signal(barrier, inc=1, device_id=prev_peer, device_id_type=MESH)

    loads = [
        pltpu.make_async_copy(src, dst, local_sem.at[index])
        for index, (src, dst) in enumerate(
            (
                (master_hbm, master_ref), (gate_hbm, gate_ref), (up_hbm, up_ref), (cot_hbm, cot_ref),
                (one_hbm, one_ref), (two_hbm, two_ref),
            )
        )
    ]
    for load in loads:
        load.start()
    loads[0].wait()
    weights[me] = master_ref[...].astype(jnp.bfloat16)
    pl.semaphore_wait(barrier, 3 + has_next.astype(jnp.int32) + has_prev.astype(jnp.int32))

    def w_go(slot, which, device, cond=None, inside=None):
        def ends():
            ref = weights.at[slot, :, parts[which]]
            return ref, ref, w_recv.at[which, slot]

        go(ends, device, cond, inside)

    def w_wait(slot, which):
        ref = weights.at[slot, :, parts[which]]
        remote(ref, ref, send_sem.at[0], w_recv.at[which, slot], core_peer).wait_recv()

    w_go(me, 1, mid_peer)
    w_go(me, 0, next_peer, has_next)
    w_go(me, 0, prev_peer, has_prev)
    w_go(me, 1, next_peer, has_next)
    w_go(me, 1, prev_peer, has_prev)
    w_go(me, 0, mid_peer)
    w_go(me, 1, core_peer)
    w_go(me, 0, core_peer)

    def along(k, m, which):
        for cond, slot, device, more in (
            (out >= k, at(out - k, m, core), next_peer, has_next),
            (out + k <= last, at(out + k, m, core), prev_peer, has_prev),
        ):
            @pl.when(cond)
            def _():
                w_wait(slot, which)
                w_go(slot, which, device, more, cond)
                if which == 0:
                    w_go(slot, which, mid_peer, None, cond)
                w_go(slot, which, core_peer, None, cond)

    def across_first():
        slot = at(out, 1 - mid, core)
        w_wait(slot, 1)
        w_go(slot, 1, next_peer, has_next)
        w_go(slot, 1, prev_peer, has_prev)
        w_go(slot, 1, core_peer)

    def across_last(k):
        sides = ((out >= k, out - k), (out + k <= last, out + k))
        for cond, o in sides if k else sides[:1]:
            slot = at(o, 1 - mid, core)

            @pl.when(cond)
            def _():
                w_wait(slot, 0)
                w_go(slot, 0, core_peer, None, cond)

    loads[3].wait()
    turned = jnp.transpose(cot_ref[...].astype(jnp.float32)).astype(jnp.bfloat16).reshape(n, rows, tokens)
    for o in range(outer):
        for m in range(MID):
            for c in range(CORES):
                cot_rows_ref[c, m, o] = turned[at(o, m, c)]
    go(lambda: (cot_rows_ref.at[1 - core], cot_peer, core_recv.at[0]), core_peer)
    loads[1].wait()
    loads[2].wait()

    def sweep(lo, hi, step, width=WIDTH):
        count = (hi - lo) // width

        def at_chunk(j, carry):
            step(pl.multiple_of(lo + j * width, LANES), width)
            return carry

        if count > 1:
            lax.fori_loop(0, count, at_chunk, 0)
        elif count:
            step(lo, width)
        if lo + count * width < hi:
            step(lo + count * width, hi - lo - count * width)

    def hidden_step(start, width):
        cols = pl.ds(start, width)
        gate = gate_ref[:, cols].astype(jnp.float32)
        sig = jax.nn.sigmoid(gate)
        hid[:, cols] = (gate * sig * up_ref[:, cols].astype(jnp.float32)).astype(jnp.bfloat16)

    for p, (lo, hi) in enumerate(sides):
        sweep(lo, hi, hidden_step, 2 * WIDTH)
        go(
            lambda p=p: (hid.at[:, halves[p]], hid_peer.at[:, halves[p]], core_recv.at[1 + p]),
            core_peer,
        )

    def core_wait(p):
        ref = hid_peer.at[:, halves[p]]
        remote(ref, ref, send_sem.at[0], core_recv.at[1 + p], core_peer).wait_recv()

    def grad_of(which, start, width):
        cols = pl.ds(start, width)
        own = cot_rows_ref[core, which].reshape(outer * rows, tokens)
        other = cot_peer[which].reshape(outer * rows, tokens)
        value = jnp.dot(own, hid[:, cols], preferred_element_type=jnp.float32)
        value += jnp.dot(other, hid_peer[:, cols], preferred_element_type=jnp.float32)
        return value.reshape(outer, rows, width)

    def send_step(start, width):
        mid_send[:, :, pl.ds(start, width)] = grad_of(1 - mid, start, width).astype(jnp.bfloat16)

    def own_step(start, width):
        own_sum[:, :, pl.ds(start, width)] = grad_of(mid, start, width)

    def wide_columns(start, width):
        return pl.ds(pl.multiple_of(start - early, LANES), width)

    def wide_step(start, width):
        for m in range(MID):
            wide_sum[m, :, :, wide_columns(start, width)] = grad_of(m, start, width)

    def target(i):
        if i == last:
            return out
        down = last - i
        down = jnp.where(down <= out, down - 1, down)
        return jnp.where(low, down, jnp.where(i >= out, i + 1, i))

    def reduce_across(i, h):
        t = target(i)
        go(
            lambda: (mid_send.at[t, :, pieces[h]], mid_recv.at[t, :, pieces[h]], mid_recv_sem.at[h, t]),
            mid_peer,
        )

    def mid_wait(t, h):
        ref = mid_recv.at[t, :, pieces[h]]
        remote(ref, ref, send_sem.at[0], mid_recv_sem.at[h, t], mid_peer).wait_recv()

    def line_wait(d, t, h):
        ref = line_recv.at[d, t, :, pieces[h]]
        remote(ref, ref, send_sem.at[0], line_recv_sem.at[d, h, t], mid_peer).wait_recv()

    def pass_on(i, h, cond=None):
        t = target(i)
        d = jnp.where(t > out, 0, 1)
        more = jnp.where(t > out, has_prev, has_next)
        lo, hi = bounds[h]
        toward = {"dp": at(out + 1 - 2 * d, mid, core)}

        def step(chained):
            def inner(start, width):
                cols = pl.ds(start, width)
                value = own_sum[t, :, cols] + mid_recv[t, :, cols].astype(jnp.float32)
                if chained:
                    value += line_recv[d, t, :, cols].astype(jnp.float32)
                line_send[t, :, cols] = value.astype(jnp.bfloat16)

            return inner

        def run():
            mid_wait(t, h)

            @pl.when(more)
            def _():
                line_wait(d, t, h)
                sweep(lo, hi, step(True))

            @pl.when(jnp.logical_not(more))
            def _():
                sweep(lo, hi, step(False))

            go(
                lambda: (
                    line_send.at[t, :, pieces[h]], line_recv.at[d, t, :, pieces[h]],
                    line_recv_sem.at[d, h, t],
                ),
                toward, None, cond,
            )

        if cond is None:
            run()
        else:
            pl.when(cond)(run)

    def wide_wait(d, m, t):
        ref = wide_recv.at[d, m, t]
        remote(ref, ref, send_sem.at[0], wide_recv_sem.at[d, m, t], mid_peer).wait_recv()

    def wide_on(i, p, cond=None):
        t = target(i)
        m = mid if p else 1 - mid
        d = jnp.where(t > out, 0, 1)
        more = jnp.where(t > out, has_prev, has_next)
        toward = {"dp": at(out + 1 - 2 * d, mid, core)}

        def step(chained):
            def inner(start, width):
                cols = wide_columns(start, width)
                value = wide_sum[m, t, :, cols]
                if chained:
                    value += wide_recv[d, m, t, :, cols].astype(jnp.float32)
                wide_send[m, t, :, cols] = value.astype(jnp.bfloat16)

            return inner

        def run():
            @pl.when(more)
            def _():
                wide_wait(d, m, t)
                sweep(early, ff, step(True))

            @pl.when(jnp.logical_not(more))
            def _():
                sweep(early, ff, step(False))

            go(
                lambda: (wide_send.at[m, t], wide_recv.at[d, m, t], wide_recv_sem.at[d, m, t]),
                toward, None, cond,
            )

        if cond is None:
            run()
        else:
            pl.when(cond)(run)

    def wide_total(m, cols):
        value = wide_sum[m, out, :, cols]
        value += wide_recv[0, m, out, :, cols].astype(jnp.float32)
        return value + wide_recv[1, m, out, :, cols].astype(jnp.float32)

    def wide_arrived(m):
        pl.when(has_prev)(lambda: wide_wait(0, m, out))
        pl.when(has_next)(lambda: wide_wait(1, m, out))

    def wide_across():
        wide_arrived(1 - mid)

        def step(start, width):
            cols = wide_columns(start, width)
            cross_send[:, cols] = wide_total(1 - mid, cols).astype(jnp.bfloat16)

        sweep(early, ff, step)
        go(lambda: (cross_send, cross_recv, cross_recv_sem), mid_peer)

    @pl.when(jnp.logical_not(has_prev))
    def _():
        line_recv[0, out] = jnp.zeros((rows, early), jnp.bfloat16)
        wide_recv[0, :, out] = jnp.zeros((MID, rows, ff - early), jnp.bfloat16)

    @pl.when(jnp.logical_not(has_next))
    def _():
        line_recv[1, out] = jnp.zeros((rows, early), jnp.bfloat16)
        wide_recv[1, :, out] = jnp.zeros((MID, rows, ff - early), jnp.bfloat16)

    def nearest(j):
        if j == 0:
            return out
        k = (j + 1) // 2
        z = jnp.where(low, out, last - out)
        g = jnp.where(j <= 2 * z, z - k if j % 2 else z + k, j)
        return jnp.where(low, g, last - g)

    half = outer // 2
    deep = block * rows

    def use_block(j):
        g = nearest(j)
        for m in range(MID):
            for which in range(2):
                w_wait(at(g, m, 1 - core), which)
        some = weights[pl.ds(g * block, block)].reshape(deep, ff)
        value = lax.dot_general(hid[...], some, (((1,), (1,)), ((), ())), preferred_element_type=jnp.float32)
        part[g] = value
        part_send[g] = value.astype(jnp.bfloat16)
        place = lax.rem(g, half)
        go(
            lambda: (part_send.at[g], part_recv.at[place], part_recv_sem.at[place]),
            rep_peer, g // half != rep,
        )
        cot = cot_ref[:, pl.ds(pl.multiple_of(g * deep, deep), deep)]

        def step(start, width):
            cols = pl.ds(start, width)
            grad = jnp.dot(
                cot, weights[pl.ds(g * block, block), :, cols].reshape(deep, width),
                preferred_element_type=jnp.float32,
            )
            if j > 0:
                grad += hid_grad[:, cols]
            if j < last:
                hid_grad[:, cols] = grad
            else:
                gate = gate_ref[:, cols].astype(jnp.float32)
                up_val = up_ref[:, cols].astype(jnp.float32)
                sig = jax.nn.sigmoid(gate)
                gate_grad_ref[:, cols] = (grad * up_val * sig * (1.0 + gate * (1.0 - sig))).astype(jnp.bfloat16)
                up_grad_ref[:, cols] = (grad * gate * sig).astype(jnp.bfloat16)

        sweep(0, ff, step, ff if j < last else BROAD)

    edge = jnp.logical_or(out == 0, out == last)
    inner = jnp.logical_not(edge)
    loads[4].wait()
    loads[5].wait()

    def update_step(total_of):
        def step(start, width):
            cols = pl.ds(start, width)
            master_new, moment, square = adam(
                total_of(start, width) / jnp.float32(total),
                master_ref[:, cols], one_ref[:, cols], two_ref[:, cols],
            )
            master_new_ref[:, cols] = master_new
            first_ref[:, cols] = moment
            second_ref[:, cols] = square

        return step

    def early_total(start, width):
        cols = pl.ds(start, width)
        value = own_sum[out, :, cols] + mid_recv[out, :, cols].astype(jnp.float32)
        return value + line_recv[0, out, :, cols].astype(jnp.float32) + line_recv[1, out, :, cols].astype(jnp.float32)

    def late_total(start, width):
        cols = wide_columns(start, width)
        return wide_total(mid, cols) + cross_recv[:, cols].astype(jnp.float32)

    def own_done(h):
        pl.when(has_prev)(lambda: line_wait(0, out, h))
        pl.when(has_next)(lambda: line_wait(1, out, h))
        mid_wait(out, h)
        sweep(*bounds[h], update_step(early_total))

    def wide_done():
        wide_arrived(mid)
        remote(cross_recv, cross_recv, send_sem.at[0], cross_recv_sem, mid_peer).wait_recv()
        sweep(early, ff, update_step(late_total))

    def core_ready(p):
        if p == 0:
            remote(cot_peer, cot_peer, send_sem.at[0], core_recv.at[0], core_peer).wait_recv()
        core_wait(p)

    acts = {
        "core": core_ready,
        "wide": lambda: sweep(early, ff, wide_step, BROAD),
        "send": lambda: sweep(0, early, send_step, 2 * BROAD),
        "own": lambda: sweep(0, early, own_step, 2 * BROAD),
        "along": lambda k, other, which: along(k, 1 - mid if other else mid, which),
        "first": across_first,
        "last": across_last,
        "across": reduce_across,
        "edge": lambda i, h: pass_on(i, h, edge),
        "inner": lambda i, h: pass_on(i, h, inner),
        "wedge": lambda i, p: wide_on(i, p, edge),
        "winner": lambda i, p: wide_on(i, p, inner),
        "cross": wide_across,
        "block": use_block,
        "fin": own_done,
        "finw": wide_done,
    }
    for name, *given in ORDER:
        acts[name](*given)

    for place in range(half):
        ref = part_recv.at[place]
        remote(ref, ref, send_sem.at[0], part_recv_sem.at[place], rep_peer).wait_recv()
        out_ref[:, place * deep : (place + 1) * deep] = (
            part[rep * half + place] + part_recv[place].astype(jnp.float32)
        ).astype(jnp.bfloat16)
    for make, given in started:
        if given:
            pl.when(functools.reduce(jnp.logical_and, given))(lambda: make().wait_send())
        else:
            make().wait_send()


def handed_on(values):
    count = len(values)

    def body(*refs):
        sems = refs[-1]
        copies = [
            pltpu.make_async_copy(refs[index], refs[count + index], sems.at[index]) for index in range(count)
        ]
        for copy in copies:
            copy.start()
        for copy in copies:
            copy.wait()

    return pl.pallas_call(
        body,
        out_shape=[jax.ShapeDtypeStruct(value.shape, value.dtype) for value in values],
        in_specs=[pl.BlockSpec(memory_space=pltpu.VMEM)] * count,
        out_specs=[pl.BlockSpec(memory_space=pl.ANY)] * count,
        scratch_shapes=[pltpu.SemaphoreType.DMA((count,))],
        compiler_params=pltpu.CompilerParams(vmem_limit_bytes=8 * 1024 * 1024),
    )(*[pltpu.with_memory_space_constraint(value, pltpu.VMEM) for value in values])


def in_one_kernel(size, gate_pre, up_pre, out_grad, master, moment_one, moment_two):
    micro, count, ff = gate_pre.shape
    tokens, depth, rows = micro * count, out_grad.shape[2], master.shape[0]
    outer = size // (MID * CORES)
    deep = MID * CORES * rows
    split = max(1, round(ff * ALONG / 128)) * 128
    early = max(1, round(ff * ACROSS / LANES)) * LANES
    cot = out_grad.reshape(tokens, depth)
    hbm = pl.BlockSpec(memory_space=pl.ANY)
    bf, f32 = jnp.bfloat16, jnp.float32
    dma = pltpu.SemaphoreType.DMA
    results = pl.pallas_call(
        functools.partial(fused, outer, tokens * size, split, early),
        out_shape=(
            pltpu.VMEM((tokens, depth // 2), bf),
            pltpu.VMEM((tokens, ff), bf),
            pltpu.VMEM((tokens, ff), bf),
            pltpu.VMEM((rows, ff), f32),
            pltpu.VMEM((rows, ff), f32),
            pltpu.VMEM((rows, ff), f32),
        ),
        in_specs=[hbm] * 6,
        out_specs=(pl.BlockSpec(memory_space=pltpu.VMEM),) * 6,
        scratch_shapes=[
            pltpu.VMEM((size, rows, ff), bf),
            pltpu.VMEM((tokens, ff), bf),
            pltpu.VMEM((tokens, ff), bf),
            pltpu.VMEM((MID, outer, rows, tokens), bf),
            pltpu.VMEM((outer, rows, early), f32),
            pltpu.VMEM((outer, rows, early), bf),
            pltpu.VMEM((outer, rows, early), bf),
            pltpu.VMEM((outer, rows, early), bf),
            pltpu.VMEM((2, outer, rows, early), bf),
            pltpu.VMEM((MID, outer, rows, ff - early), f32),
            pltpu.VMEM((MID, outer, rows, ff - early), bf),
            pltpu.VMEM((2, MID, outer, rows, ff - early), bf),
            pltpu.VMEM((rows, ff - early), bf),
            pltpu.VMEM((rows, ff - early), bf),
            pltpu.VMEM((outer, tokens, deep), f32),
            pltpu.VMEM((outer, tokens, deep), bf),
            pltpu.VMEM((outer // 2, tokens, deep), bf),
            pltpu.VMEM((tokens, ff), f32),
            pltpu.VMEM((CORES, MID, outer, rows, tokens), bf),
            pltpu.VMEM((tokens, ff), bf),
            pltpu.VMEM((tokens, ff), bf),
            pltpu.VMEM((tokens, depth), bf),
            pltpu.VMEM((rows, ff), f32),
            pltpu.VMEM((rows, ff), f32),
            pltpu.VMEM((rows, ff), f32),
            dma((6,)), dma((40 * outer,)), dma((2, size)), dma((3,)),
            dma((2, outer)), dma((2, 2, outer)), dma((2, MID, outer)), dma, dma((outer // 2,)),
        ],
        compiler_params=pltpu.CompilerParams(
            collective_id=0, has_side_effects=True, vmem_limit_bytes=50 * 1024 * 1024
        ),
    )(
        gate_pre.reshape(tokens, ff), up_pre.reshape(tokens, ff), cot, master, moment_one, moment_two,
    )
    results = handed_on(results)
    split = [value.reshape(micro, count, value.shape[1]) for value in results[:3]]
    return (*split, *results[3:])


def with_collectives(gate_pre, up_pre, out_grad, master, moment_one, moment_two):
    weights = lax.all_gather(master.astype(jnp.bfloat16), "dp", axis=0, tiled=True)
    micro = gate_pre.shape[0]
    total = micro * gate_pre.shape[1] * lax.axis_size("dp")
    outs_list = []
    gate_list = []
    up_list = []
    grad_sum = None
    for index in range(micro):
        gate = gate_pre[index].astype(jnp.float32)
        up_val = up_pre[index].astype(jnp.float32)
        sig = jax.nn.sigmoid(gate)
        hidden = (gate * sig * up_val).astype(jnp.bfloat16)
        partial_out = lax.dot_general(
            hidden, weights, (((1,), (1,)), ((), ())), preferred_element_type=jnp.float32
        )
        outs_list.append(
            lax.psum_scatter(partial_out, "rep", scatter_dimension=1, tiled=True).astype(
                jnp.bfloat16
            )
        )
        hid_grad = jnp.dot(out_grad[index], weights, preferred_element_type=jnp.float32)
        gate_list.append(
            (hid_grad * up_val * sig * (1.0 + gate * (1.0 - sig))).astype(jnp.bfloat16)
        )
        up_list.append((hid_grad * gate * sig).astype(jnp.bfloat16))
        term = lax.dot_general(
            out_grad[index], hidden, (((0,), (0,)), ((), ())), preferred_element_type=jnp.float32
        )
        shard = lax.psum_scatter(term, "dp", scatter_dimension=0, tiled=True)
        grad_sum = shard if grad_sum is None else grad_sum + shard
    updated = adam(grad_sum / jnp.float32(total), master, moment_one, moment_two)
    return jnp.stack(outs_list), jnp.stack(gate_list), jnp.stack(up_list), *updated


def solution(mesh):
    size = mesh.shape["dp"]

    def on_device(gate_pre, up_pre, out_grad, master, moment_one, moment_two):
        line = size == LINE * MID * CORES
        tall = line and master.shape[0] % 32 == 0 and master.shape[1] % LANES == 0 and master.shape[1] >= 8 * LANES
        step = functools.partial(in_one_kernel, size) if tall else with_collectives
        return step(gate_pre, up_pre, out_grad, master, moment_one, moment_two)

    split = P(None, "dp", "rep")
    owned = P("dp", "rep")
    return jax.shard_map(
        on_device,
        mesh=mesh,
        in_specs=(split, split, P(None, "dp", None), owned, owned, owned),
        out_specs=(split, split, split, owned, owned, owned),
        check_vma=False,
    )
```

```python
import functools

import jax
import jax.numpy as jnp
from jax import lax
from jax.experimental import pallas as pl
from jax.experimental.pallas import tpu as pltpu
from jax.sharding import PartitionSpec as P

first_power = 2.6561398887587544e-05
second_power = 0.005920529220333997

MESH = pl.DeviceIdType.MESH
CORES = 2
MID = 2
LINE = 4
LANES = 128
WIDTH = 256
BROAD = 1408
ALONG = 0.636
ACROSS = 0.545
LEAD = 0.500
ORDER = (
    ("core", 0), ("core", 1), ("first",), ("send",), ("along", 1, 0, 0), ("wide",), ("across", 1, 1),
    ("across", 0, 1), ("last", 0), ("wedge", 0, 0), ("along", 1, 0, 1), ("along", 1, 1, 1), ("wedge", 1, 0),
    ("wedge", 2, 0), ("across", 0, 0), ("winner", 0, 0), ("wedge", 0, 1), ("along", 2, 0, 0), ("own",),
    ("last", 1), ("across", 1, 0), ("across", 2, 1), ("edge", 0, 1), ("edge", 0, 0), ("along", 2, 1, 1),
    ("edge", 1, 1), ("winner", 1, 0), ("across", 2, 0), ("wedge", 1, 1), ("winner", 2, 0), ("along", 3, 0, 0),
    ("edge", 1, 0), ("winner", 0, 1), ("along", 2, 0, 1), ("block", 0), ("inner", 0, 1), ("block", 1),
    ("inner", 0, 0), ("last", 2), ("across", 3, 1), ("block", 2), ("winner", 2, 1), ("inner", 1, 1),
    ("inner", 2, 1), ("cross",), ("wedge", 2, 1), ("edge", 2, 1), ("across", 3, 0), ("along", 3, 1, 1),
    ("last", 3), ("edge", 2, 0), ("winner", 1, 1), ("along", 3, 0, 1), ("inner", 2, 0), ("block", 3),
    ("inner", 1, 0), ("finw",), ("fin", 1), ("fin", 0),
)


def adam(main_grad, master, moment_one, moment_two):
    first = 0.9 * moment_one + 0.1 * main_grad
    second = 0.95 * moment_two + 0.05 * main_grad * main_grad
    update = first / (1.0 - first_power) / (jnp.sqrt(second / (1.0 - second_power)) + 1e-08)
    return master - 0.003 * (update + 0.1 * master), first, second


def fused(
    outer, total, split, early,
    gate_hbm, up_hbm, cot_hbm, master_hbm, one_hbm, two_hbm,
    out_ref, gate_grad_ref, up_grad_ref, master_new_ref, first_ref, second_ref,
    weights, hid, hid_peer, cot_peer, own_sum, mid_send, mid_recv, line_send, line_recv,
    wide_sum, wide_send, wide_recv, cross_send, cross_recv,
    part, part_send, part_recv, hid_grad, cot_rows_ref,
    gate_ref, up_ref, cot_ref, master_ref, one_ref, two_ref,
    local_sem, send_sem, w_recv, core_recv, mid_recv_sem, line_recv_sem, wide_recv_sem, cross_recv_sem, part_recv_sem,
):
    me = lax.axis_index("dp")
    rep = lax.axis_index("rep")
    core = lax.rem(me, CORES)
    mid = lax.rem(me // CORES, MID)
    out = me // (CORES * MID)
    n = outer * MID * CORES
    block = MID * CORES
    rows, ff = master_ref.shape
    tokens = gate_ref.shape[0]
    lead = max(1, round(early * LEAD / LANES)) * LANES
    bounds = ((0, lead), (lead, early))
    pieces = tuple(pl.ds(lo, hi - lo) for lo, hi in bounds)
    sides = ((early, ff), (0, early))
    halves = tuple(pl.ds(lo, hi - lo) for lo, hi in sides)
    parts = (pl.ds(0, split), pl.ds(split, ff - split))
    last = outer - 1
    low = out < outer // 2

    def at(o, m, c):
        return (o * MID + m) * CORES + c

    core_peer = {"dp": at(out, mid, 1 - core)}
    mid_peer = {"dp": at(out, 1 - mid, core)}
    rep_peer = {"rep": 1 - rep}
    next_peer = {"dp": at(jnp.minimum(out + 1, last), mid, core)}
    prev_peer = {"dp": at(jnp.maximum(out - 1, 0), mid, core)}
    has_next = out < last
    has_prev = out > 0

    def remote(src, dst, send, recv, device):
        return pltpu.make_async_remote_copy(
            src_ref=src, dst_ref=dst, send_sem=send, recv_sem=recv,
            device_id=device, device_id_type=MESH,
        )

    started = []

    def go(ends, device, cond=None, inside=None):
        index = len(started)

        def make():
            src, dst, recv = ends()
            return remote(src, dst, send_sem.at[index], recv, device)

        if cond is None:
            make().start()
        else:
            pl.when(cond)(lambda: make().start())
        started.append((make, [given for given in (inside, cond) if given is not None]))

    barrier = pltpu.get_barrier_semaphore()
    for peer in (core_peer, mid_peer, rep_peer):
        pl.semaphore_signal(barrier, inc=1, device_id=peer, device_id_type=MESH)

    @pl.when(has_next)
    def _():
        pl.semaphore_signal(barrier, inc=1, device_id=next_peer, device_id_type=MESH)

    @pl.when(has_prev)
    def _():
        pl.semaphore_signal(barrier, inc=1, device_id=prev_peer, device_id_type=MESH)

    loads = [
        pltpu.make_async_copy(src, dst, local_sem.at[index])
        for index, (src, dst) in enumerate(
            (
                (master_hbm, master_ref), (gate_hbm, gate_ref), (up_hbm, up_ref), (cot_hbm, cot_ref),
                (one_hbm, one_ref), (two_hbm, two_ref),
            )
        )
    ]
    for load in loads:
        load.start()
    loads[0].wait()
    weights[me] = master_ref[...].astype(jnp.bfloat16)
    pl.semaphore_wait(barrier, 3 + has_next.astype(jnp.int32) + has_prev.astype(jnp.int32))

    def w_go(slot, which, device, cond=None, inside=None):
        def ends():
            ref = weights.at[slot, :, parts[which]]
            return ref, ref, w_recv.at[which, slot]

        go(ends, device, cond, inside)

    def w_wait(slot, which):
        ref = weights.at[slot, :, parts[which]]
        remote(ref, ref, send_sem.at[0], w_recv.at[which, slot], core_peer).wait_recv()

    w_go(me, 1, mid_peer)
    w_go(me, 0, next_peer, has_next)
    w_go(me, 0, prev_peer, has_prev)
    w_go(me, 1, next_peer, has_next)
    w_go(me, 1, prev_peer, has_prev)
    w_go(me, 0, mid_peer)
    w_go(me, 1, core_peer)
    w_go(me, 0, core_peer)

    def along(k, m, which):
        for cond, slot, device, more in (
            (out >= k, at(out - k, m, core), next_peer, has_next),
            (out + k <= last, at(out + k, m, core), prev_peer, has_prev),
        ):
            @pl.when(cond)
            def _():
                w_wait(slot, which)
                w_go(slot, which, device, more, cond)
                if which == 0:
                    w_go(slot, which, mid_peer, None, cond)
                w_go(slot, which, core_peer, None, cond)

    def across_first():
        slot = at(out, 1 - mid, core)
        w_wait(slot, 1)
        w_go(slot, 1, next_peer, has_next)
        w_go(slot, 1, prev_peer, has_prev)
        w_go(slot, 1, core_peer)

    def across_last(k):
        sides = ((out >= k, out - k), (out + k <= last, out + k))
        for cond, o in sides if k else sides[:1]:
            slot = at(o, 1 - mid, core)

            @pl.when(cond)
            def _():
                w_wait(slot, 0)
                w_go(slot, 0, core_peer, None, cond)

    loads[3].wait()
    turned = jnp.transpose(cot_ref[...].astype(jnp.float32)).astype(jnp.bfloat16).reshape(n, rows, tokens)
    for o in range(outer):
        for m in range(MID):
            for c in range(CORES):
                cot_rows_ref[c, m, o] = turned[at(o, m, c)]
    go(lambda: (cot_rows_ref.at[1 - core], cot_peer, core_recv.at[0]), core_peer)
    loads[1].wait()
    loads[2].wait()

    def sweep(lo, hi, step, width=WIDTH):
        count = (hi - lo) // width

        def at_chunk(j, carry):
            step(pl.multiple_of(lo + j * width, LANES), width)
            return carry

        if count > 1:
            lax.fori_loop(0, count, at_chunk, 0)
        elif count:
            step(lo, width)
        if lo + count * width < hi:
            step(lo + count * width, hi - lo - count * width)

    def hidden_step(start, width):
        cols = pl.ds(start, width)
        gate = gate_ref[:, cols].astype(jnp.float32)
        sig = jax.nn.sigmoid(gate)
        hid[:, cols] = (gate * sig * up_ref[:, cols].astype(jnp.float32)).astype(jnp.bfloat16)

    for p, (lo, hi) in enumerate(sides):
        sweep(lo, hi, hidden_step, 2 * WIDTH)
        go(
            lambda p=p: (hid.at[:, halves[p]], hid_peer.at[:, halves[p]], core_recv.at[1 + p]),
            core_peer,
        )

    def core_wait(p):
        ref = hid_peer.at[:, halves[p]]
        remote(ref, ref, send_sem.at[0], core_recv.at[1 + p], core_peer).wait_recv()

    def grad_of(which, start, width):
        cols = pl.ds(start, width)
        own = cot_rows_ref[core, which].reshape(outer * rows, tokens)
        other = cot_peer[which].reshape(outer * rows, tokens)
        value = jnp.dot(own, hid[:, cols], preferred_element_type=jnp.float32)
        value += jnp.dot(other, hid_peer[:, cols], preferred_element_type=jnp.float32)
        return value.reshape(outer, rows, width)

    def send_step(start, width):
        mid_send[:, :, pl.ds(start, width)] = grad_of(1 - mid, start, width).astype(jnp.bfloat16)

    def own_step(start, width):
        own_sum[:, :, pl.ds(start, width)] = grad_of(mid, start, width)

    def wide_columns(start, width):
        return pl.ds(pl.multiple_of(start - early, LANES), width)

    def wide_step(start, width):
        for m in range(MID):
            wide_sum[m, :, :, wide_columns(start, width)] = grad_of(m, start, width)

    def target(i):
        if i == last:
            return out
        down = last - i
        down = jnp.where(down <= out, down - 1, down)
        return jnp.where(low, down, jnp.where(i >= out, i + 1, i))

    def reduce_across(i, h):
        t = target(i)
        go(
            lambda: (mid_send.at[t, :, pieces[h]], mid_recv.at[t, :, pieces[h]], mid_recv_sem.at[h, t]),
            mid_peer,
        )

    def mid_wait(t, h):
        ref = mid_recv.at[t, :, pieces[h]]
        remote(ref, ref, send_sem.at[0], mid_recv_sem.at[h, t], mid_peer).wait_recv()

    def line_wait(d, t, h):
        ref = line_recv.at[d, t, :, pieces[h]]
        remote(ref, ref, send_sem.at[0], line_recv_sem.at[d, h, t], mid_peer).wait_recv()

    def pass_on(i, h, cond=None):
        t = target(i)
        d = jnp.where(t > out, 0, 1)
        more = jnp.where(t > out, has_prev, has_next)
        lo, hi = bounds[h]
        toward = {"dp": at(out + 1 - 2 * d, mid, core)}

        def step(chained):
            def inner(start, width):
                cols = pl.ds(start, width)
                value = own_sum[t, :, cols] + mid_recv[t, :, cols].astype(jnp.float32)
                if chained:
                    value += line_recv[d, t, :, cols].astype(jnp.float32)
                line_send[t, :, cols] = value.astype(jnp.bfloat16)

            return inner

        def run():
            mid_wait(t, h)

            @pl.when(more)
            def _():
                line_wait(d, t, h)
                sweep(lo, hi, step(True))

            @pl.when(jnp.logical_not(more))
            def _():
                sweep(lo, hi, step(False))

            go(
                lambda: (
                    line_send.at[t, :, pieces[h]], line_recv.at[d, t, :, pieces[h]],
                    line_recv_sem.at[d, h, t],
                ),
                toward, None, cond,
            )

        if cond is None:
            run()
        else:
            pl.when(cond)(run)

    def wide_wait(d, m, t):
        ref = wide_recv.at[d, m, t]
        remote(ref, ref, send_sem.at[0], wide_recv_sem.at[d, m, t], mid_peer).wait_recv()

    def wide_on(i, p, cond=None):
        t = target(i)
        m = mid if p else 1 - mid
        d = jnp.where(t > out, 0, 1)
        more = jnp.where(t > out, has_prev, has_next)
        toward = {"dp": at(out + 1 - 2 * d, mid, core)}

        def step(chained):
            def inner(start, width):
                cols = wide_columns(start, width)
                value = wide_sum[m, t, :, cols]
                if chained:
                    value += wide_recv[d, m, t, :, cols].astype(jnp.float32)
                wide_send[m, t, :, cols] = value.astype(jnp.bfloat16)

            return inner

        def run():
            @pl.when(more)
            def _():
                wide_wait(d, m, t)
                sweep(early, ff, step(True))

            @pl.when(jnp.logical_not(more))
            def _():
                sweep(early, ff, step(False))

            go(
                lambda: (wide_send.at[m, t], wide_recv.at[d, m, t], wide_recv_sem.at[d, m, t]),
                toward, None, cond,
            )

        if cond is None:
            run()
        else:
            pl.when(cond)(run)

    def wide_total(m, cols):
        value = wide_sum[m, out, :, cols]
        value += wide_recv[0, m, out, :, cols].astype(jnp.float32)
        return value + wide_recv[1, m, out, :, cols].astype(jnp.float32)

    def wide_arrived(m):
        pl.when(has_prev)(lambda: wide_wait(0, m, out))
        pl.when(has_next)(lambda: wide_wait(1, m, out))

    def wide_across():
        wide_arrived(1 - mid)

        def step(start, width):
            cols = wide_columns(start, width)
            cross_send[:, cols] = wide_total(1 - mid, cols).astype(jnp.bfloat16)

        sweep(early, ff, step)
        go(lambda: (cross_send, cross_recv, cross_recv_sem), mid_peer)

    @pl.when(jnp.logical_not(has_prev))
    def _():
        line_recv[0, out] = jnp.zeros((rows, early), jnp.bfloat16)
        wide_recv[0, :, out] = jnp.zeros((MID, rows, ff - early), jnp.bfloat16)

    @pl.when(jnp.logical_not(has_next))
    def _():
        line_recv[1, out] = jnp.zeros((rows, early), jnp.bfloat16)
        wide_recv[1, :, out] = jnp.zeros((MID, rows, ff - early), jnp.bfloat16)

    def nearest(j):
        if j == 0:
            return out
        k = (j + 1) // 2
        z = jnp.where(low, out, last - out)
        g = jnp.where(j <= 2 * z, z - k if j % 2 else z + k, j)
        return jnp.where(low, g, last - g)

    half = outer // 2
    deep = block * rows

    def use_block(j):
        g = nearest(j)
        for m in range(MID):
            for which in range(2):
                w_wait(at(g, m, 1 - core), which)
        some = weights[pl.ds(g * block, block)].reshape(deep, ff)
        value = lax.dot_general(hid[...], some, (((1,), (1,)), ((), ())), preferred_element_type=jnp.float32)
        part[g] = value
        part_send[g] = value.astype(jnp.bfloat16)
        place = lax.rem(g, half)
        go(
            lambda: (part_send.at[g], part_recv.at[place], part_recv_sem.at[place]),
            rep_peer, g // half != rep,
        )
        cot = cot_ref[:, pl.ds(pl.multiple_of(g * deep, deep), deep)]

        def step(start, width):
            cols = pl.ds(start, width)
            grad = jnp.dot(
                cot, weights[pl.ds(g * block, block), :, cols].reshape(deep, width),
                preferred_element_type=jnp.float32,
            )
            if j > 0:
                grad += hid_grad[:, cols]
            if j < last:
                hid_grad[:, cols] = grad
            else:
                gate = gate_ref[:, cols].astype(jnp.float32)
                up_val = up_ref[:, cols].astype(jnp.float32)
                sig = jax.nn.sigmoid(gate)
                gate_grad_ref[:, cols] = (grad * up_val * sig * (1.0 + gate * (1.0 - sig))).astype(jnp.bfloat16)
                up_grad_ref[:, cols] = (grad * gate * sig).astype(jnp.bfloat16)

        sweep(0, ff, step, ff if j < last else BROAD)

    edge = jnp.logical_or(out == 0, out == last)
    inner = jnp.logical_not(edge)
    loads[4].wait()
    loads[5].wait()

    def update_step(total_of):
        def step(start, width):
            cols = pl.ds(start, width)
            master_new, moment, square = adam(
                total_of(start, width) / jnp.float32(total),
                master_ref[:, cols], one_ref[:, cols], two_ref[:, cols],
            )
            master_new_ref[:, cols] = master_new
            first_ref[:, cols] = moment
            second_ref[:, cols] = square

        return step

    def early_total(start, width):
        cols = pl.ds(start, width)
        value = own_sum[out, :, cols] + mid_recv[out, :, cols].astype(jnp.float32)
        return value + line_recv[0, out, :, cols].astype(jnp.float32) + line_recv[1, out, :, cols].astype(jnp.float32)

    def late_total(start, width):
        cols = wide_columns(start, width)
        return wide_total(mid, cols) + cross_recv[:, cols].astype(jnp.float32)

    def own_done(h):
        pl.when(has_prev)(lambda: line_wait(0, out, h))
        pl.when(has_next)(lambda: line_wait(1, out, h))
        mid_wait(out, h)
        sweep(*bounds[h], update_step(early_total))

    def wide_done():
        wide_arrived(mid)
        remote(cross_recv, cross_recv, send_sem.at[0], cross_recv_sem, mid_peer).wait_recv()
        sweep(early, ff, update_step(late_total))

    def core_ready(p):
        if p == 0:
            remote(cot_peer, cot_peer, send_sem.at[0], core_recv.at[0], core_peer).wait_recv()
        core_wait(p)

    acts = {
        "core": core_ready,
        "wide": lambda: sweep(early, ff, wide_step, BROAD),
        "send": lambda: sweep(0, early, send_step, 2 * BROAD),
        "own": lambda: sweep(0, early, own_step, 2 * BROAD),
        "along": lambda k, other, which: along(k, 1 - mid if other else mid, which),
        "first": across_first,
        "last": across_last,
        "across": reduce_across,
        "edge": lambda i, h: pass_on(i, h, edge),
        "inner": lambda i, h: pass_on(i, h, inner),
        "wedge": lambda i, p: wide_on(i, p, edge),
        "winner": lambda i, p: wide_on(i, p, inner),
        "cross": wide_across,
        "block": use_block,
        "fin": own_done,
        "finw": wide_done,
    }
    for name, *given in ORDER:
        acts[name](*given)

    for place in range(half):
        ref = part_recv.at[place]
        remote(ref, ref, send_sem.at[0], part_recv_sem.at[place], rep_peer).wait_recv()
        out_ref[:, place * deep : (place + 1) * deep] = (
            part[rep * half + place] + part_recv[place].astype(jnp.float32)
        ).astype(jnp.bfloat16)
    for make, given in started:
        if given:
            pl.when(functools.reduce(jnp.logical_and, given))(lambda: make().wait_send())
        else:
            make().wait_send()


def handed_on(values):
    count = len(values)

    def body(*refs):
        sems = refs[-1]
        copies = [
            pltpu.make_async_copy(refs[index], refs[count + index], sems.at[index]) for index in range(count)
        ]
        for copy in copies:
            copy.start()
        for copy in copies:
            copy.wait()

    return pl.pallas_call(
        body,
        out_shape=[jax.ShapeDtypeStruct(value.shape, value.dtype) for value in values],
        in_specs=[pl.BlockSpec(memory_space=pltpu.VMEM)] * count,
        out_specs=[pl.BlockSpec(memory_space=pl.ANY)] * count,
        scratch_shapes=[pltpu.SemaphoreType.DMA((count,))],
        compiler_params=pltpu.CompilerParams(vmem_limit_bytes=8 * 1024 * 1024),
    )(*[pltpu.with_memory_space_constraint(value, pltpu.VMEM) for value in values])


def in_one_kernel(size, gate_pre, up_pre, out_grad, master, moment_one, moment_two):
    micro, count, ff = gate_pre.shape
    tokens, depth, rows = micro * count, out_grad.shape[2], master.shape[0]
    outer = size // (MID * CORES)
    deep = MID * CORES * rows
    split = max(1, round(ff * ALONG / 128)) * 128
    early = max(1, round(ff * ACROSS / LANES)) * LANES
    cot = out_grad.reshape(tokens, depth)
    hbm = pl.BlockSpec(memory_space=pl.ANY)
    bf, f32 = jnp.bfloat16, jnp.float32
    dma = pltpu.SemaphoreType.DMA
    results = pl.pallas_call(
        functools.partial(fused, outer, tokens * size, split, early),
        out_shape=(
            pltpu.VMEM((tokens, depth // 2), bf),
            pltpu.VMEM((tokens, ff), bf),
            pltpu.VMEM((tokens, ff), bf),
            pltpu.VMEM((rows, ff), f32),
            pltpu.VMEM((rows, ff), f32),
            pltpu.VMEM((rows, ff), f32),
        ),
        in_specs=[hbm] * 6,
        out_specs=(pl.BlockSpec(memory_space=pltpu.VMEM),) * 6,
        scratch_shapes=[
            pltpu.VMEM((size, rows, ff), bf),
            pltpu.VMEM((tokens, ff), bf),
            pltpu.VMEM((tokens, ff), bf),
            pltpu.VMEM((MID, outer, rows, tokens), bf),
            pltpu.VMEM((outer, rows, early), f32),
            pltpu.VMEM((outer, rows, early), bf),
            pltpu.VMEM((outer, rows, early), bf),
            pltpu.VMEM((outer, rows, early), bf),
            pltpu.VMEM((2, outer, rows, early), bf),
            pltpu.VMEM((MID, outer, rows, ff - early), f32),
            pltpu.VMEM((MID, outer, rows, ff - early), bf),
            pltpu.VMEM((2, MID, outer, rows, ff - early), bf),
            pltpu.VMEM((rows, ff - early), bf),
            pltpu.VMEM((rows, ff - early), bf),
            pltpu.VMEM((outer, tokens, deep), f32),
            pltpu.VMEM((outer, tokens, deep), bf),
            pltpu.VMEM((outer // 2, tokens, deep), bf),
            pltpu.VMEM((tokens, ff), f32),
            pltpu.VMEM((CORES, MID, outer, rows, tokens), bf),
            pltpu.VMEM((tokens, ff), bf),
            pltpu.VMEM((tokens, ff), bf),
            pltpu.VMEM((tokens, depth), bf),
            pltpu.VMEM((rows, ff), f32),
            pltpu.VMEM((rows, ff), f32),
            pltpu.VMEM((rows, ff), f32),
            dma((6,)), dma((40 * outer,)), dma((2, size)), dma((3,)),
            dma((2, outer)), dma((2, 2, outer)), dma((2, MID, outer)), dma, dma((outer // 2,)),
        ],
        compiler_params=pltpu.CompilerParams(
            collective_id=0, has_side_effects=True, vmem_limit_bytes=50 * 1024 * 1024
        ),
    )(
        gate_pre.reshape(tokens, ff), up_pre.reshape(tokens, ff), cot, master, moment_one, moment_two,
    )
    results = handed_on(results)
    split = [value.reshape(micro, count, value.shape[1]) for value in results[:3]]
    return (*split, *results[3:])


def with_collectives(gate_pre, up_pre, out_grad, master, moment_one, moment_two):
    weights = lax.all_gather(master.astype(jnp.bfloat16), "dp", axis=0, tiled=True)
    micro = gate_pre.shape[0]
    total = micro * gate_pre.shape[1] * lax.axis_size("dp")
    outs_list = []
    gate_list = []
    up_list = []
    grad_sum = None
    for index in range(micro):
        gate = gate_pre[index].astype(jnp.float32)
        up_val = up_pre[index].astype(jnp.float32)
        sig = jax.nn.sigmoid(gate)
        hidden = (gate * sig * up_val).astype(jnp.bfloat16)
        partial_out = lax.dot_general(
            hidden, weights, (((1,), (1,)), ((), ())), preferred_element_type=jnp.float32
        )
        outs_list.append(
            lax.psum_scatter(partial_out, "rep", scatter_dimension=1, tiled=True).astype(
                jnp.bfloat16
            )
        )
        hid_grad = jnp.dot(out_grad[index], weights, preferred_element_type=jnp.float32)
        gate_list.append(
            (hid_grad * up_val * sig * (1.0 + gate * (1.0 - sig))).astype(jnp.bfloat16)
        )
        up_list.append((hid_grad * gate * sig).astype(jnp.bfloat16))
        term = lax.dot_general(
            out_grad[index], hidden, (((0,), (0,)), ((), ())), preferred_element_type=jnp.float32
        )
        shard = lax.psum_scatter(term, "dp", scatter_dimension=0, tiled=True)
        grad_sum = shard if grad_sum is None else grad_sum + shard
    updated = adam(grad_sum / jnp.float32(total), master, moment_one, moment_two)
    return jnp.stack(outs_list), jnp.stack(gate_list), jnp.stack(up_list), *updated


def solution(mesh):
    size = mesh.shape["dp"]

    def on_device(gate_pre, up_pre, out_grad, master, moment_one, moment_two):
        line = size == LINE * MID * CORES
        tall = line and master.shape[0] % 32 == 0 and master.shape[1] % LANES == 0 and master.shape[1] >= 8 * LANES
        step = functools.partial(in_one_kernel, size) if tall else with_collectives
        return step(gate_pre, up_pre, out_grad, master, moment_one, moment_two)

    split = P(None, "dp", "rep")
    owned = P("dp", "rep")
    return jax.shard_map(
        on_device,
        mesh=mesh,
        in_specs=(split, split, P(None, "dp", None), owned, owned, owned),
        out_specs=(split, split, split, owned, owned, owned),
        check_vma=False,
    )
```

```python
import functools

import jax
import jax.numpy as jnp
from jax import lax
from jax.experimental import pallas as pl
from jax.experimental.pallas import tpu as pltpu
from jax.sharding import PartitionSpec as P

first_power = 2.6561398887587544e-05
second_power = 0.005920529220333997

MESH = pl.DeviceIdType.MESH
CORES = 2
MID = 2
LINE = 4
LANES = 128
WIDTH = 256
BROAD = 1408
ALONG = 0.636
ACROSS = 0.545
LEAD = 0.500
ORDER = (
    ("core", 0), ("core", 1), ("first",), ("send",), ("along", 1, 0, 0), ("wide",), ("across", 1, 1),
    ("across", 0, 1), ("last", 0), ("wedge", 0, 0), ("along", 1, 0, 1), ("along", 1, 1, 1), ("wedge", 1, 0),
    ("wedge", 2, 0), ("across", 0, 0), ("winner", 0, 0), ("wedge", 0, 1), ("along", 2, 0, 0), ("own",),
    ("last", 1), ("across", 1, 0), ("across", 2, 1), ("edge", 0, 1), ("edge", 0, 0), ("along", 2, 1, 1),
    ("edge", 1, 1), ("winner", 1, 0), ("across", 2, 0), ("wedge", 1, 1), ("winner", 2, 0), ("along", 3, 0, 0),
    ("edge", 1, 0), ("winner", 0, 1), ("along", 2, 0, 1), ("block", 0), ("inner", 0, 1), ("block", 1),
    ("inner", 0, 0), ("last", 2), ("across", 3, 1), ("block", 2), ("winner", 2, 1), ("inner", 1, 1),
    ("inner", 2, 1), ("cross",), ("wedge", 2, 1), ("edge", 2, 1), ("across", 3, 0), ("along", 3, 1, 1),
    ("last", 3), ("edge", 2, 0), ("winner", 1, 1), ("along", 3, 0, 1), ("inner", 2, 0), ("block", 3),
    ("inner", 1, 0), ("finw",), ("fin", 1), ("fin", 0),
)


def adam(main_grad, master, moment_one, moment_two):
    first = 0.9 * moment_one + 0.1 * main_grad
    second = 0.95 * moment_two + 0.05 * main_grad * main_grad
    update = first * (1.0 / (1.0 - first_power)) / (jnp.sqrt(second * (1.0 / (1.0 - second_power))) + 1e-08)
    return master - 0.003 * (update + 0.1 * master), first, second


def fused(
    outer, total, split, early,
    gate_hbm, up_hbm, cot_hbm, master_hbm, one_hbm, two_hbm,
    out_ref, gate_grad_ref, up_grad_ref, master_new_ref, first_ref, second_ref,
    weights, hid, hid_peer, cot_peer, own_sum, mid_send, mid_recv, line_send, line_recv,
    wide_sum, wide_send, wide_recv, cross_send, cross_recv,
    part, part_send, part_recv, hid_grad, cot_rows_ref,
    gate_ref, up_ref, cot_ref, master_ref, one_ref, two_ref,
    local_sem, send_sem, w_recv, core_recv, mid_recv_sem, line_recv_sem, wide_recv_sem, cross_recv_sem, part_recv_sem,
):
    me = lax.axis_index("dp")
    rep = lax.axis_index("rep")
    core = lax.rem(me, CORES)
    mid = lax.rem(me // CORES, MID)
    out = me // (CORES * MID)
    n = outer * MID * CORES
    block = MID * CORES
    rows, ff = master_ref.shape
    tokens = gate_ref.shape[0]
    lead = max(1, round(early * LEAD / LANES)) * LANES
    bounds = ((0, lead), (lead, early))
    pieces = tuple(pl.ds(lo, hi - lo) for lo, hi in bounds)
    sides = ((early, ff), (0, early))
    halves = tuple(pl.ds(lo, hi - lo) for lo, hi in sides)
    parts = (pl.ds(0, split), pl.ds(split, ff - split))
    last = outer - 1
    low = out < outer // 2

    def at(o, m, c):
        return (o * MID + m) * CORES + c

    core_peer = {"dp": at(out, mid, 1 - core)}
    mid_peer = {"dp": at(out, 1 - mid, core)}
    rep_peer = {"rep": 1 - rep}
    next_peer = {"dp": at(jnp.minimum(out + 1, last), mid, core)}
    prev_peer = {"dp": at(jnp.maximum(out - 1, 0), mid, core)}
    has_next = out < last
    has_prev = out > 0

    def remote(src, dst, send, recv, device):
        return pltpu.make_async_remote_copy(
            src_ref=src, dst_ref=dst, send_sem=send, recv_sem=recv,
            device_id=device, device_id_type=MESH,
        )

    started = []

    def go(ends, device, cond=None, inside=None):
        index = len(started)

        def make():
            src, dst, recv = ends()
            return remote(src, dst, send_sem.at[index], recv, device)

        if cond is None:
            make().start()
        else:
            pl.when(cond)(lambda: make().start())
        started.append((make, [given for given in (inside, cond) if given is not None]))

    barrier = pltpu.get_barrier_semaphore()
    for peer in (core_peer, mid_peer, rep_peer):
        pl.semaphore_signal(barrier, inc=1, device_id=peer, device_id_type=MESH)

    @pl.when(has_next)
    def _():
        pl.semaphore_signal(barrier, inc=1, device_id=next_peer, device_id_type=MESH)

    @pl.when(has_prev)
    def _():
        pl.semaphore_signal(barrier, inc=1, device_id=prev_peer, device_id_type=MESH)

    loads = [
        pltpu.make_async_copy(src, dst, local_sem.at[index])
        for index, (src, dst) in enumerate(
            (
                (master_hbm, master_ref), (gate_hbm, gate_ref), (up_hbm, up_ref), (cot_hbm, cot_ref),
                (one_hbm, one_ref), (two_hbm, two_ref),
            )
        )
    ]
    for load in loads:
        load.start()
    loads[0].wait()
    weights[me] = master_ref[...].astype(jnp.bfloat16)
    pl.semaphore_wait(barrier, 3 + has_next.astype(jnp.int32) + has_prev.astype(jnp.int32))

    def w_go(slot, which, device, cond=None, inside=None):
        def ends():
            ref = weights.at[slot, :, parts[which]]
            return ref, ref, w_recv.at[which, slot]

        go(ends, device, cond, inside)

    def w_wait(slot, which):
        ref = weights.at[slot, :, parts[which]]
        remote(ref, ref, send_sem.at[0], w_recv.at[which, slot], core_peer).wait_recv()

    w_go(me, 1, mid_peer)
    w_go(me, 0, next_peer, has_next)
    w_go(me, 0, prev_peer, has_prev)
    w_go(me, 1, next_peer, has_next)
    w_go(me, 1, prev_peer, has_prev)
    w_go(me, 0, mid_peer)
    w_go(me, 1, core_peer)
    w_go(me, 0, core_peer)

    def along(k, m, which):
        for cond, slot, device, more in (
            (out >= k, at(out - k, m, core), next_peer, has_next),
            (out + k <= last, at(out + k, m, core), prev_peer, has_prev),
        ):
            @pl.when(cond)
            def _():
                w_wait(slot, which)
                w_go(slot, which, device, more, cond)
                if which == 0:
                    w_go(slot, which, mid_peer, None, cond)
                w_go(slot, which, core_peer, None, cond)

    def across_first():
        slot = at(out, 1 - mid, core)
        w_wait(slot, 1)
        w_go(slot, 1, next_peer, has_next)
        w_go(slot, 1, prev_peer, has_prev)
        w_go(slot, 1, core_peer)

    def across_last(k):
        sides = ((out >= k, out - k), (out + k <= last, out + k))
        for cond, o in sides if k else sides[:1]:
            slot = at(o, 1 - mid, core)

            @pl.when(cond)
            def _():
                w_wait(slot, 0)
                w_go(slot, 0, core_peer, None, cond)

    loads[3].wait()
    turned = jnp.transpose(cot_ref[...].astype(jnp.float32)).astype(jnp.bfloat16).reshape(n, rows, tokens)
    for o in range(outer):
        for m in range(MID):
            for c in range(CORES):
                cot_rows_ref[c, m, o] = turned[at(o, m, c)]
    go(lambda: (cot_rows_ref.at[1 - core], cot_peer, core_recv.at[0]), core_peer)
    loads[1].wait()
    loads[2].wait()

    def sweep(lo, hi, step, width=WIDTH):
        count = (hi - lo) // width

        def at_chunk(j, carry):
            step(pl.multiple_of(lo + j * width, LANES), width)
            return carry

        if count > 1:
            lax.fori_loop(0, count, at_chunk, 0)
        elif count:
            step(lo, width)
        if lo + count * width < hi:
            step(lo + count * width, hi - lo - count * width)

    def hidden_step(start, width):
        cols = pl.ds(start, width)
        gate = gate_ref[:, cols].astype(jnp.float32)
        sig = jax.nn.sigmoid(gate)
        hid[:, cols] = (gate * sig * up_ref[:, cols].astype(jnp.float32)).astype(jnp.bfloat16)

    for p, (lo, hi) in enumerate(sides):
        sweep(lo, hi, hidden_step, 2 * WIDTH)
        go(
            lambda p=p: (hid.at[:, halves[p]], hid_peer.at[:, halves[p]], core_recv.at[1 + p]),
            core_peer,
        )

    def core_wait(p):
        ref = hid_peer.at[:, halves[p]]
        remote(ref, ref, send_sem.at[0], core_recv.at[1 + p], core_peer).wait_recv()

    def grad_of(which, start, width):
        cols = pl.ds(start, width)
        own = cot_rows_ref[core, which].reshape(outer * rows, tokens)
        other = cot_peer[which].reshape(outer * rows, tokens)
        value = jnp.dot(own, hid[:, cols], preferred_element_type=jnp.float32)
        value += jnp.dot(other, hid_peer[:, cols], preferred_element_type=jnp.float32)
        return value.reshape(outer, rows, width)

    def send_step(start, width):
        mid_send[:, :, pl.ds(start, width)] = grad_of(1 - mid, start, width).astype(jnp.bfloat16)

    def own_step(start, width):
        own_sum[:, :, pl.ds(start, width)] = grad_of(mid, start, width)

    def wide_columns(start, width):
        return pl.ds(pl.multiple_of(start - early, LANES), width)

    def wide_step(start, width):
        for m in range(MID):
            wide_sum[m, :, :, wide_columns(start, width)] = grad_of(m, start, width)

    def target(i):
        if i == last:
            return out
        down = last - i
        down = jnp.where(down <= out, down - 1, down)
        return jnp.where(low, down, jnp.where(i >= out, i + 1, i))

    def reduce_across(i, h):
        t = target(i)
        go(
            lambda: (mid_send.at[t, :, pieces[h]], mid_recv.at[t, :, pieces[h]], mid_recv_sem.at[h, t]),
            mid_peer,
        )

    def mid_wait(t, h):
        ref = mid_recv.at[t, :, pieces[h]]
        remote(ref, ref, send_sem.at[0], mid_recv_sem.at[h, t], mid_peer).wait_recv()

    def line_wait(d, t, h):
        ref = line_recv.at[d, t, :, pieces[h]]
        remote(ref, ref, send_sem.at[0], line_recv_sem.at[d, h, t], mid_peer).wait_recv()

    def pass_on(i, h, cond=None):
        t = target(i)
        d = jnp.where(t > out, 0, 1)
        more = jnp.where(t > out, has_prev, has_next)
        lo, hi = bounds[h]
        toward = {"dp": at(out + 1 - 2 * d, mid, core)}

        def step(chained):
            def inner(start, width):
                cols = pl.ds(start, width)
                value = own_sum[t, :, cols] + mid_recv[t, :, cols].astype(jnp.float32)
                if chained:
                    value += line_recv[d, t, :, cols].astype(jnp.float32)
                line_send[t, :, cols] = value.astype(jnp.bfloat16)

            return inner

        def run():
            mid_wait(t, h)

            @pl.when(more)
            def _():
                line_wait(d, t, h)
                sweep(lo, hi, step(True))

            @pl.when(jnp.logical_not(more))
            def _():
                sweep(lo, hi, step(False))

            go(
                lambda: (
                    line_send.at[t, :, pieces[h]], line_recv.at[d, t, :, pieces[h]],
                    line_recv_sem.at[d, h, t],
                ),
                toward, None, cond,
            )

        if cond is None:
            run()
        else:
            pl.when(cond)(run)

    def wide_wait(d, m, t):
        ref = wide_recv.at[d, m, t]
        remote(ref, ref, send_sem.at[0], wide_recv_sem.at[d, m, t], mid_peer).wait_recv()

    def wide_on(i, p, cond=None):
        t = target(i)
        m = mid if p else 1 - mid
        d = jnp.where(t > out, 0, 1)
        more = jnp.where(t > out, has_prev, has_next)
        toward = {"dp": at(out + 1 - 2 * d, mid, core)}

        def step(chained):
            def inner(start, width):
                cols = wide_columns(start, width)
                value = wide_sum[m, t, :, cols]
                if chained:
                    value += wide_recv[d, m, t, :, cols].astype(jnp.float32)
                wide_send[m, t, :, cols] = value.astype(jnp.bfloat16)

            return inner

        def run():
            @pl.when(more)
            def _():
                wide_wait(d, m, t)
                sweep(early, ff, step(True))

            @pl.when(jnp.logical_not(more))
            def _():
                sweep(early, ff, step(False))

            go(
                lambda: (wide_send.at[m, t], wide_recv.at[d, m, t], wide_recv_sem.at[d, m, t]),
                toward, None, cond,
            )

        if cond is None:
            run()
        else:
            pl.when(cond)(run)

    def wide_total(m, cols):
        value = wide_sum[m, out, :, cols]
        value += wide_recv[0, m, out, :, cols].astype(jnp.float32)
        return value + wide_recv[1, m, out, :, cols].astype(jnp.float32)

    def wide_arrived(m):
        pl.when(has_prev)(lambda: wide_wait(0, m, out))
        pl.when(has_next)(lambda: wide_wait(1, m, out))

    def wide_across():
        wide_arrived(1 - mid)

        def step(start, width):
            cols = wide_columns(start, width)
            cross_send[:, cols] = wide_total(1 - mid, cols).astype(jnp.bfloat16)

        sweep(early, ff, step)
        go(lambda: (cross_send, cross_recv, cross_recv_sem), mid_peer)

    @pl.when(jnp.logical_not(has_prev))
    def _():
        line_recv[0, out] = jnp.zeros((rows, early), jnp.bfloat16)
        wide_recv[0, :, out] = jnp.zeros((MID, rows, ff - early), jnp.bfloat16)

    @pl.when(jnp.logical_not(has_next))
    def _():
        line_recv[1, out] = jnp.zeros((rows, early), jnp.bfloat16)
        wide_recv[1, :, out] = jnp.zeros((MID, rows, ff - early), jnp.bfloat16)

    def nearest(j):
        if j == 0:
            return out
        k = (j + 1) // 2
        z = jnp.where(low, out, last - out)
        g = jnp.where(j <= 2 * z, z - k if j % 2 else z + k, j)
        return jnp.where(low, g, last - g)

    half = outer // 2
    deep = block * rows

    def use_block(j):
        g = nearest(j)
        for m in range(MID):
            for which in range(2):
                w_wait(at(g, m, 1 - core), which)
        some = weights[pl.ds(g * block, block)].reshape(deep, ff)
        value = lax.dot_general(hid[...], some, (((1,), (1,)), ((), ())), preferred_element_type=jnp.float32)
        part[g] = value
        part_send[g] = value.astype(jnp.bfloat16)
        place = lax.rem(g, half)
        go(
            lambda: (part_send.at[g], part_recv.at[place], part_recv_sem.at[place]),
            rep_peer, g // half != rep,
        )
        cot = cot_ref[:, pl.ds(pl.multiple_of(g * deep, deep), deep)]

        def step(start, width):
            cols = pl.ds(start, width)
            grad = jnp.dot(
                cot, weights[pl.ds(g * block, block), :, cols].reshape(deep, width),
                preferred_element_type=jnp.float32,
            )
            if j > 0:
                grad += hid_grad[:, cols]
            if j < last:
                hid_grad[:, cols] = grad
            else:
                gate = gate_ref[:, cols].astype(jnp.float32)
                up_val = up_ref[:, cols].astype(jnp.float32)
                sig = jax.nn.sigmoid(gate)
                gate_grad_ref[:, cols] = (grad * up_val * sig * (1.0 + gate * (1.0 - sig))).astype(jnp.bfloat16)
                up_grad_ref[:, cols] = (grad * gate * sig).astype(jnp.bfloat16)

        sweep(0, ff, step, ff if j < last else BROAD)

    edge = jnp.logical_or(out == 0, out == last)
    inner = jnp.logical_not(edge)
    loads[4].wait()
    loads[5].wait()

    def update_step(total_of):
        def step(start, width):
            cols = pl.ds(start, width)
            master_new, moment, square = adam(
                total_of(start, width) * jnp.float32(1.0 / total),
                master_ref[:, cols], one_ref[:, cols], two_ref[:, cols],
            )
            master_new_ref[:, cols] = master_new
            first_ref[:, cols] = moment
            second_ref[:, cols] = square

        return step

    def early_total(start, width):
        cols = pl.ds(start, width)
        value = own_sum[out, :, cols] + mid_recv[out, :, cols].astype(jnp.float32)
        return value + line_recv[0, out, :, cols].astype(jnp.float32) + line_recv[1, out, :, cols].astype(jnp.float32)

    def late_total(start, width):
        cols = wide_columns(start, width)
        return wide_total(mid, cols) + cross_recv[:, cols].astype(jnp.float32)

    def own_done(h):
        pl.when(has_prev)(lambda: line_wait(0, out, h))
        pl.when(has_next)(lambda: line_wait(1, out, h))
        mid_wait(out, h)
        sweep(*bounds[h], update_step(early_total))

    def wide_done():
        wide_arrived(mid)
        remote(cross_recv, cross_recv, send_sem.at[0], cross_recv_sem, mid_peer).wait_recv()
        sweep(early, ff, update_step(late_total))

    def core_ready(p):
        if p == 0:
            remote(cot_peer, cot_peer, send_sem.at[0], core_recv.at[0], core_peer).wait_recv()
        core_wait(p)

    acts = {
        "core": core_ready,
        "wide": lambda: sweep(early, ff, wide_step, BROAD),
        "send": lambda: sweep(0, early, send_step, 2 * BROAD),
        "own": lambda: sweep(0, early, own_step, 2 * BROAD),
        "along": lambda k, other, which: along(k, 1 - mid if other else mid, which),
        "first": across_first,
        "last": across_last,
        "across": reduce_across,
        "edge": lambda i, h: pass_on(i, h, edge),
        "inner": lambda i, h: pass_on(i, h, inner),
        "wedge": lambda i, p: wide_on(i, p, edge),
        "winner": lambda i, p: wide_on(i, p, inner),
        "cross": wide_across,
        "block": use_block,
        "fin": own_done,
        "finw": wide_done,
    }
    def settle():
        for place in range(half):
            ref = part_recv.at[place]
            remote(ref, ref, send_sem.at[0], part_recv_sem.at[place], rep_peer).wait_recv()
            out_ref[:, place * deep : (place + 1) * deep] = (
                part[rep * half + place] + part_recv[place].astype(jnp.float32)
            ).astype(jnp.bfloat16)
        for make, given in started:
            if given:
                pl.when(functools.reduce(jnp.logical_and, given))(lambda: make().wait_send())
            else:
                make().wait_send()

    for name, *given in ORDER[:-1]:
        acts[name](*given)
    settle()
    for name, *given in ORDER[-1:]:
        acts[name](*given)


def handed_on(values):
    count = len(values)

    def body(*refs):
        sems = refs[-1]
        copies = [
            pltpu.make_async_copy(refs[index], refs[count + index], sems.at[index]) for index in range(count)
        ]
        for copy in copies:
            copy.start()
        for copy in copies:
            copy.wait()

    return pl.pallas_call(
        body,
        out_shape=[jax.ShapeDtypeStruct(value.shape, value.dtype) for value in values],
        in_specs=[pl.BlockSpec(memory_space=pltpu.VMEM)] * count,
        out_specs=[pl.BlockSpec(memory_space=pl.ANY)] * count,
        scratch_shapes=[pltpu.SemaphoreType.DMA((count,))],
        compiler_params=pltpu.CompilerParams(vmem_limit_bytes=8 * 1024 * 1024),
    )(*[pltpu.with_memory_space_constraint(value, pltpu.VMEM) for value in values])


def in_one_kernel(size, gate_pre, up_pre, out_grad, master, moment_one, moment_two):
    micro, count, ff = gate_pre.shape
    tokens, depth, rows = micro * count, out_grad.shape[2], master.shape[0]
    outer = size // (MID * CORES)
    deep = MID * CORES * rows
    split = max(1, round(ff * ALONG / 128)) * 128
    early = max(1, round(ff * ACROSS / LANES)) * LANES
    cot = out_grad.reshape(tokens, depth)
    hbm = pl.BlockSpec(memory_space=pl.ANY)
    bf, f32 = jnp.bfloat16, jnp.float32
    dma = pltpu.SemaphoreType.DMA
    results = pl.pallas_call(
        functools.partial(fused, outer, tokens * size, split, early),
        out_shape=(
            pltpu.VMEM((tokens, depth // 2), bf),
            pltpu.VMEM((tokens, ff), bf),
            pltpu.VMEM((tokens, ff), bf),
            pltpu.VMEM((rows, ff), f32),
            pltpu.VMEM((rows, ff), f32),
            pltpu.VMEM((rows, ff), f32),
        ),
        in_specs=[hbm] * 6,
        out_specs=(pl.BlockSpec(memory_space=pltpu.VMEM),) * 6,
        scratch_shapes=[
            pltpu.VMEM((size, rows, ff), bf),
            pltpu.VMEM((tokens, ff), bf),
            pltpu.VMEM((tokens, ff), bf),
            pltpu.VMEM((MID, outer, rows, tokens), bf),
            pltpu.VMEM((outer, rows, early), f32),
            pltpu.VMEM((outer, rows, early), bf),
            pltpu.VMEM((outer, rows, early), bf),
            pltpu.VMEM((outer, rows, early), bf),
            pltpu.VMEM((2, outer, rows, early), bf),
            pltpu.VMEM((MID, outer, rows, ff - early), f32),
            pltpu.VMEM((MID, outer, rows, ff - early), bf),
            pltpu.VMEM((2, MID, outer, rows, ff - early), bf),
            pltpu.VMEM((rows, ff - early), bf),
            pltpu.VMEM((rows, ff - early), bf),
            pltpu.VMEM((outer, tokens, deep), f32),
            pltpu.VMEM((outer, tokens, deep), bf),
            pltpu.VMEM((outer // 2, tokens, deep), bf),
            pltpu.VMEM((tokens, ff), f32),
            pltpu.VMEM((CORES, MID, outer, rows, tokens), bf),
            pltpu.VMEM((tokens, ff), bf),
            pltpu.VMEM((tokens, ff), bf),
            pltpu.VMEM((tokens, depth), bf),
            pltpu.VMEM((rows, ff), f32),
            pltpu.VMEM((rows, ff), f32),
            pltpu.VMEM((rows, ff), f32),
            dma((6,)), dma((40 * outer,)), dma((2, size)), dma((3,)),
            dma((2, outer)), dma((2, 2, outer)), dma((2, MID, outer)), dma, dma((outer // 2,)),
        ],
        compiler_params=pltpu.CompilerParams(
            collective_id=0, has_side_effects=True, vmem_limit_bytes=50 * 1024 * 1024
        ),
    )(
        gate_pre.reshape(tokens, ff), up_pre.reshape(tokens, ff), cot, master, moment_one, moment_two,
    )
    results = handed_on(results)
    split = [value.reshape(micro, count, value.shape[1]) for value in results[:3]]
    return (*split, *results[3:])


def with_collectives(gate_pre, up_pre, out_grad, master, moment_one, moment_two):
    weights = lax.all_gather(master.astype(jnp.bfloat16), "dp", axis=0, tiled=True)
    micro = gate_pre.shape[0]
    total = micro * gate_pre.shape[1] * lax.axis_size("dp")
    outs_list = []
    gate_list = []
    up_list = []
    grad_sum = None
    for index in range(micro):
        gate = gate_pre[index].astype(jnp.float32)
        up_val = up_pre[index].astype(jnp.float32)
        sig = jax.nn.sigmoid(gate)
        hidden = (gate * sig * up_val).astype(jnp.bfloat16)
        partial_out = lax.dot_general(
            hidden, weights, (((1,), (1,)), ((), ())), preferred_element_type=jnp.float32
        )
        outs_list.append(
            lax.psum_scatter(partial_out, "rep", scatter_dimension=1, tiled=True).astype(
                jnp.bfloat16
            )
        )
        hid_grad = jnp.dot(out_grad[index], weights, preferred_element_type=jnp.float32)
        gate_list.append(
            (hid_grad * up_val * sig * (1.0 + gate * (1.0 - sig))).astype(jnp.bfloat16)
        )
        up_list.append((hid_grad * gate * sig).astype(jnp.bfloat16))
        term = lax.dot_general(
            out_grad[index], hidden, (((0,), (0,)), ((), ())), preferred_element_type=jnp.float32
        )
        shard = lax.psum_scatter(term, "dp", scatter_dimension=0, tiled=True)
        grad_sum = shard if grad_sum is None else grad_sum + shard
    updated = adam(grad_sum / jnp.float32(total), master, moment_one, moment_two)
    return jnp.stack(outs_list), jnp.stack(gate_list), jnp.stack(up_list), *updated


def solution(mesh):
    size = mesh.shape["dp"]

    def on_device(gate_pre, up_pre, out_grad, master, moment_one, moment_two):
        line = size == LINE * MID * CORES
        tall = line and master.shape[0] % 32 == 0 and master.shape[1] % LANES == 0 and master.shape[1] >= 8 * LANES
        step = functools.partial(in_one_kernel, size) if tall else with_collectives
        return step(gate_pre, up_pre, out_grad, master, moment_one, moment_two)

    split = P(None, "dp", "rep")
    owned = P("dp", "rep")
    return jax.shard_map(
        on_device,
        mesh=mesh,
        in_specs=(split, split, P(None, "dp", None), owned, owned, owned),
        out_specs=(split, split, split, owned, owned, owned),
        check_vma=False,
    )
```

```python
import functools

import jax
import jax.numpy as jnp
from jax import lax
from jax.experimental import pallas as pl
from jax.experimental.pallas import tpu as pltpu
from jax.sharding import PartitionSpec as P

first_power = 2.6561398887587544e-05
second_power = 0.005920529220333997

MESH = pl.DeviceIdType.MESH
CORES = 2
MID = 2
LINE = 4
LANES = 128
WIDTH = 256
BROAD = 1408
ALONG = 0.636
ACROSS = 0.545
LEAD = 0.333
ORDER = (
    ("core", 0), ("core", 1), ("first",), ("send",), ("along", 1, 0, 0), ("wide",), ("across", 1, 1),
    ("across", 0, 1), ("last", 0), ("wedge", 0, 0), ("along", 1, 0, 1), ("along", 1, 1, 1), ("wedge", 1, 0),
    ("wedge", 2, 0), ("across", 0, 0), ("winner", 0, 0), ("wedge", 0, 1), ("along", 2, 0, 0), ("own",),
    ("last", 1), ("across", 1, 0), ("across", 2, 1), ("edge", 0, 1), ("edge", 0, 0), ("along", 2, 1, 1),
    ("edge", 1, 1), ("winner", 1, 0), ("across", 2, 0), ("wedge", 1, 1), ("winner", 2, 0), ("along", 3, 0, 0),
    ("edge", 1, 0), ("winner", 0, 1), ("along", 2, 0, 1), ("block", 0), ("inner", 0, 1), ("block", 1),
    ("inner", 0, 0), ("last", 2), ("across", 3, 1), ("block", 2), ("winner", 2, 1), ("inner", 1, 1),
    ("inner", 2, 1), ("cross",), ("wedge", 2, 1), ("edge", 2, 1), ("across", 3, 0), ("along", 3, 1, 1),
    ("last", 3), ("edge", 2, 0), ("winner", 1, 1), ("along", 3, 0, 1), ("inner", 2, 0), ("block", 3),
    ("inner", 1, 0), ("finw",), ("fin", 1), ("fin", 0),
)


def adam(main_grad, master, moment_one, moment_two):
    first = 0.9 * moment_one + 0.1 * main_grad
    second = 0.95 * moment_two + 0.05 * main_grad * main_grad
    update = first * (1.0 / (1.0 - first_power)) / (jnp.sqrt(second * (1.0 / (1.0 - second_power))) + 1e-08)
    return master - 0.003 * (update + 0.1 * master), first, second


def fused(
    outer, total, split, early,
    gate_hbm, up_hbm, cot_hbm, master_hbm, one_hbm, two_hbm,
    out_ref, gate_grad_ref, up_grad_ref, master_new_ref, first_ref, second_ref,
    weights, hid, hid_peer, cot_peer, own_sum, mid_send, mid_recv, line_send, line_recv,
    wide_sum, wide_send, wide_recv, cross_send, cross_recv,
    part, part_send, part_recv, hid_grad, cot_rows_ref,
    gate_ref, up_ref, cot_ref, master_ref, one_ref, two_ref,
    local_sem, send_sem, w_recv, core_recv, mid_recv_sem, line_recv_sem, wide_recv_sem, cross_recv_sem, part_recv_sem,
):
    me = lax.axis_index("dp")
    rep = lax.axis_index("rep")
    core = lax.rem(me, CORES)
    mid = lax.rem(me // CORES, MID)
    out = me // (CORES * MID)
    n = outer * MID * CORES
    block = MID * CORES
    rows, ff = master_ref.shape
    tokens = gate_ref.shape[0]
    lead = max(1, round(early * LEAD / LANES)) * LANES
    bounds = ((0, lead), (lead, early))
    pieces = tuple(pl.ds(lo, hi - lo) for lo, hi in bounds)
    sides = ((early, ff), (0, early))
    halves = tuple(pl.ds(lo, hi - lo) for lo, hi in sides)
    parts = (pl.ds(0, split), pl.ds(split, ff - split))
    last = outer - 1
    low = out < outer // 2

    def at(o, m, c):
        return (o * MID + m) * CORES + c

    core_peer = {"dp": at(out, mid, 1 - core)}
    mid_peer = {"dp": at(out, 1 - mid, core)}
    rep_peer = {"rep": 1 - rep}
    next_peer = {"dp": at(jnp.minimum(out + 1, last), mid, core)}
    prev_peer = {"dp": at(jnp.maximum(out - 1, 0), mid, core)}
    has_next = out < last
    has_prev = out > 0

    def remote(src, dst, send, recv, device):
        return pltpu.make_async_remote_copy(
            src_ref=src, dst_ref=dst, send_sem=send, recv_sem=recv,
            device_id=device, device_id_type=MESH,
        )

    started = []

    def go(ends, device, cond=None, inside=None):
        index = len(started)

        def make():
            src, dst, recv = ends()
            return remote(src, dst, send_sem.at[index], recv, device)

        if cond is None:
            make().start()
        else:
            pl.when(cond)(lambda: make().start())
        started.append((make, [given for given in (inside, cond) if given is not None]))

    barrier = pltpu.get_barrier_semaphore()
    for peer in (core_peer, mid_peer, rep_peer):
        pl.semaphore_signal(barrier, inc=1, device_id=peer, device_id_type=MESH)

    @pl.when(has_next)
    def _():
        pl.semaphore_signal(barrier, inc=1, device_id=next_peer, device_id_type=MESH)

    @pl.when(has_prev)
    def _():
        pl.semaphore_signal(barrier, inc=1, device_id=prev_peer, device_id_type=MESH)

    loads = [
        pltpu.make_async_copy(src, dst, local_sem.at[index])
        for index, (src, dst) in enumerate(
            (
                (master_hbm, master_ref), (gate_hbm, gate_ref), (up_hbm, up_ref), (cot_hbm, cot_ref),
                (one_hbm, one_ref), (two_hbm, two_ref),
            )
        )
    ]
    for load in loads:
        load.start()
    loads[0].wait()
    weights[me] = master_ref[...].astype(jnp.bfloat16)
    pl.semaphore_wait(barrier, 3 + has_next.astype(jnp.int32) + has_prev.astype(jnp.int32))

    def w_go(slot, which, device, cond=None, inside=None):
        def ends():
            ref = weights.at[slot, :, parts[which]]
            return ref, ref, w_recv.at[which, slot]

        go(ends, device, cond, inside)

    def w_wait(slot, which):
        ref = weights.at[slot, :, parts[which]]
        remote(ref, ref, send_sem.at[0], w_recv.at[which, slot], core_peer).wait_recv()

    w_go(me, 1, mid_peer)
    w_go(me, 0, next_peer, has_next)
    w_go(me, 0, prev_peer, has_prev)
    w_go(me, 1, next_peer, has_next)
    w_go(me, 1, prev_peer, has_prev)
    w_go(me, 0, mid_peer)
    w_go(me, 1, core_peer)
    w_go(me, 0, core_peer)

    def along(k, m, which):
        for cond, slot, device, more in (
            (out >= k, at(out - k, m, core), next_peer, has_next),
            (out + k <= last, at(out + k, m, core), prev_peer, has_prev),
        ):
            @pl.when(cond)
            def _():
                w_wait(slot, which)
                w_go(slot, which, device, more, cond)
                if which == 0:
                    w_go(slot, which, mid_peer, None, cond)
                w_go(slot, which, core_peer, None, cond)

    def across_first():
        slot = at(out, 1 - mid, core)
        w_wait(slot, 1)
        w_go(slot, 1, next_peer, has_next)
        w_go(slot, 1, prev_peer, has_prev)
        w_go(slot, 1, core_peer)

    def across_last(k):
        sides = ((out >= k, out - k), (out + k <= last, out + k))
        for cond, o in sides if k else sides[:1]:
            slot = at(o, 1 - mid, core)

            @pl.when(cond)
            def _():
                w_wait(slot, 0)
                w_go(slot, 0, core_peer, None, cond)

    loads[3].wait()
    turned = jnp.transpose(cot_ref[...].astype(jnp.float32)).astype(jnp.bfloat16).reshape(n, rows, tokens)
    for o in range(outer):
        for m in range(MID):
            for c in range(CORES):
                cot_rows_ref[c, m, o] = turned[at(o, m, c)]
    go(lambda: (cot_rows_ref.at[1 - core], cot_peer, core_recv.at[0]), core_peer)
    loads[1].wait()
    loads[2].wait()

    def sweep(lo, hi, step, width=WIDTH):
        count = (hi - lo) // width

        def at_chunk(j, carry):
            step(pl.multiple_of(lo + j * width, LANES), width)
            return carry

        if count > 1:
            lax.fori_loop(0, count, at_chunk, 0)
        elif count:
            step(lo, width)
        if lo + count * width < hi:
            step(lo + count * width, hi - lo - count * width)

    def hidden_step(start, width):
        cols = pl.ds(start, width)
        gate = gate_ref[:, cols].astype(jnp.float32)
        sig = jax.nn.sigmoid(gate)
        hid[:, cols] = (gate * sig * up_ref[:, cols].astype(jnp.float32)).astype(jnp.bfloat16)

    for p, (lo, hi) in enumerate(sides):
        sweep(lo, hi, hidden_step, 2 * WIDTH)
        go(
            lambda p=p: (hid.at[:, halves[p]], hid_peer.at[:, halves[p]], core_recv.at[1 + p]),
            core_peer,
        )

    def core_wait(p):
        ref = hid_peer.at[:, halves[p]]
        remote(ref, ref, send_sem.at[0], core_recv.at[1 + p], core_peer).wait_recv()

    def grad_of(which, start, width):
        cols = pl.ds(start, width)
        own = cot_rows_ref[core, which].reshape(outer * rows, tokens)
        other = cot_peer[which].reshape(outer * rows, tokens)
        value = jnp.dot(own, hid[:, cols], preferred_element_type=jnp.float32)
        value += jnp.dot(other, hid_peer[:, cols], preferred_element_type=jnp.float32)
        return value.reshape(outer, rows, width)

    def send_step(start, width):
        mid_send[:, :, pl.ds(start, width)] = grad_of(1 - mid, start, width).astype(jnp.bfloat16)

    def own_step(start, width):
        own_sum[:, :, pl.ds(start, width)] = grad_of(mid, start, width)

    def wide_columns(start, width):
        return pl.ds(pl.multiple_of(start - early, LANES), width)

    def wide_step(start, width):
        for m in range(MID):
            wide_sum[m, :, :, wide_columns(start, width)] = grad_of(m, start, width)

    def target(i):
        if i == last:
            return out
        down = last - i
        down = jnp.where(down <= out, down - 1, down)
        return jnp.where(low, down, jnp.where(i >= out, i + 1, i))

    def reduce_across(i, h):
        t = target(i)
        go(
            lambda: (mid_send.at[t, :, pieces[h]], mid_recv.at[t, :, pieces[h]], mid_recv_sem.at[h, t]),
            mid_peer,
        )

    def mid_wait(t, h):
        ref = mid_recv.at[t, :, pieces[h]]
        remote(ref, ref, send_sem.at[0], mid_recv_sem.at[h, t], mid_peer).wait_recv()

    def line_wait(d, t, h):
        ref = line_recv.at[d, t, :, pieces[h]]
        remote(ref, ref, send_sem.at[0], line_recv_sem.at[d, h, t], mid_peer).wait_recv()

    def pass_on(i, h, cond=None):
        t = target(i)
        d = jnp.where(t > out, 0, 1)
        more = jnp.where(t > out, has_prev, has_next)
        lo, hi = bounds[h]
        toward = {"dp": at(out + 1 - 2 * d, mid, core)}

        def step(chained):
            def inner(start, width):
                cols = pl.ds(start, width)
                value = own_sum[t, :, cols] + mid_recv[t, :, cols].astype(jnp.float32)
                if chained:
                    value += line_recv[d, t, :, cols].astype(jnp.float32)
                line_send[t, :, cols] = value.astype(jnp.bfloat16)

            return inner

        def run():
            mid_wait(t, h)

            @pl.when(more)
            def _():
                line_wait(d, t, h)
                sweep(lo, hi, step(True))

            @pl.when(jnp.logical_not(more))
            def _():
                sweep(lo, hi, step(False))

            go(
                lambda: (
                    line_send.at[t, :, pieces[h]], line_recv.at[d, t, :, pieces[h]],
                    line_recv_sem.at[d, h, t],
                ),
                toward, None, cond,
            )

        if cond is None:
            run()
        else:
            pl.when(cond)(run)

    def wide_wait(d, m, t):
        ref = wide_recv.at[d, m, t]
        remote(ref, ref, send_sem.at[0], wide_recv_sem.at[d, m, t], mid_peer).wait_recv()

    def wide_on(i, p, cond=None):
        t = target(i)
        m = mid if p else 1 - mid
        d = jnp.where(t > out, 0, 1)
        more = jnp.where(t > out, has_prev, has_next)
        toward = {"dp": at(out + 1 - 2 * d, mid, core)}

        def step(chained):
            def inner(start, width):
                cols = wide_columns(start, width)
                value = wide_sum[m, t, :, cols]
                if chained:
                    value += wide_recv[d, m, t, :, cols].astype(jnp.float32)
                wide_send[m, t, :, cols] = value.astype(jnp.bfloat16)

            return inner

        def run():
            @pl.when(more)
            def _():
                wide_wait(d, m, t)
                sweep(early, ff, step(True))

            @pl.when(jnp.logical_not(more))
            def _():
                sweep(early, ff, step(False))

            go(
                lambda: (wide_send.at[m, t], wide_recv.at[d, m, t], wide_recv_sem.at[d, m, t]),
                toward, None, cond,
            )

        if cond is None:
            run()
        else:
            pl.when(cond)(run)

    def wide_total(m, cols):
        value = wide_sum[m, out, :, cols]
        value += wide_recv[0, m, out, :, cols].astype(jnp.float32)
        return value + wide_recv[1, m, out, :, cols].astype(jnp.float32)

    def wide_arrived(m):
        pl.when(has_prev)(lambda: wide_wait(0, m, out))
        pl.when(has_next)(lambda: wide_wait(1, m, out))

    def wide_across():
        wide_arrived(1 - mid)

        def step(start, width):
            cols = wide_columns(start, width)
            cross_send[:, cols] = wide_total(1 - mid, cols).astype(jnp.bfloat16)

        sweep(early, ff, step)
        go(lambda: (cross_send, cross_recv, cross_recv_sem), mid_peer)

    @pl.when(jnp.logical_not(has_prev))
    def _():
        line_recv[0, out] = jnp.zeros((rows, early), jnp.bfloat16)
        wide_recv[0, :, out] = jnp.zeros((MID, rows, ff - early), jnp.bfloat16)

    @pl.when(jnp.logical_not(has_next))
    def _():
        line_recv[1, out] = jnp.zeros((rows, early), jnp.bfloat16)
        wide_recv[1, :, out] = jnp.zeros((MID, rows, ff - early), jnp.bfloat16)

    def nearest(j):
        if j == 0:
            return out
        k = (j + 1) // 2
        z = jnp.where(low, out, last - out)
        g = jnp.where(j <= 2 * z, z - k if j % 2 else z + k, j)
        return jnp.where(low, g, last - g)

    half = outer // 2
    deep = block * rows

    def use_block(j):
        g = nearest(j)
        for m in range(MID):
            for which in range(2):
                w_wait(at(g, m, 1 - core), which)
        some = weights[pl.ds(g * block, block)].reshape(deep, ff)
        value = lax.dot_general(hid[...], some, (((1,), (1,)), ((), ())), preferred_element_type=jnp.float32)
        part[g] = value
        part_send[g] = value.astype(jnp.bfloat16)
        place = lax.rem(g, half)
        go(
            lambda: (part_send.at[g], part_recv.at[place], part_recv_sem.at[place]),
            rep_peer, g // half != rep,
        )
        cot = cot_ref[:, pl.ds(pl.multiple_of(g * deep, deep), deep)]

        def step(start, width):
            cols = pl.ds(start, width)
            grad = jnp.dot(
                cot, weights[pl.ds(g * block, block), :, cols].reshape(deep, width),
                preferred_element_type=jnp.float32,
            )
            if j > 0:
                grad += hid_grad[:, cols]
            if j < last:
                hid_grad[:, cols] = grad
            else:
                gate = gate_ref[:, cols].astype(jnp.float32)
                up_val = up_ref[:, cols].astype(jnp.float32)
                sig = jax.nn.sigmoid(gate)
                gate_grad_ref[:, cols] = (grad * up_val * sig * (1.0 + gate * (1.0 - sig))).astype(jnp.bfloat16)
                up_grad_ref[:, cols] = (grad * gate * sig).astype(jnp.bfloat16)

        sweep(0, ff, step, ff if j < last else BROAD)

    edge = jnp.logical_or(out == 0, out == last)
    inner = jnp.logical_not(edge)
    loads[4].wait()
    loads[5].wait()

    def update_step(total_of):
        def step(start, width):
            cols = pl.ds(start, width)
            master_new, moment, square = adam(
                total_of(start, width) * jnp.float32(1.0 / total),
                master_ref[:, cols], one_ref[:, cols], two_ref[:, cols],
            )
            master_new_ref[:, cols] = master_new
            first_ref[:, cols] = moment
            second_ref[:, cols] = square

        return step

    def early_total(start, width):
        cols = pl.ds(start, width)
        value = own_sum[out, :, cols] + mid_recv[out, :, cols].astype(jnp.float32)
        return value + line_recv[0, out, :, cols].astype(jnp.float32) + line_recv[1, out, :, cols].astype(jnp.float32)

    def late_total(start, width):
        cols = wide_columns(start, width)
        return wide_total(mid, cols) + cross_recv[:, cols].astype(jnp.float32)

    def own_done(h):
        pl.when(has_prev)(lambda: line_wait(0, out, h))
        pl.when(has_next)(lambda: line_wait(1, out, h))
        mid_wait(out, h)
        sweep(*bounds[h], update_step(early_total), 2 * WIDTH)

    def wide_done():
        wide_arrived(mid)
        remote(cross_recv, cross_recv, send_sem.at[0], cross_recv_sem, mid_peer).wait_recv()
        sweep(early, ff, update_step(late_total), 2 * WIDTH)

    def core_ready(p):
        if p == 0:
            remote(cot_peer, cot_peer, send_sem.at[0], core_recv.at[0], core_peer).wait_recv()
        core_wait(p)

    acts = {
        "core": core_ready,
        "wide": lambda: sweep(early, ff, wide_step, BROAD),
        "send": lambda: sweep(0, early, send_step, 2 * BROAD),
        "own": lambda: sweep(0, early, own_step, 2 * BROAD),
        "along": lambda k, other, which: along(k, 1 - mid if other else mid, which),
        "first": across_first,
        "last": across_last,
        "across": reduce_across,
        "edge": lambda i, h: pass_on(i, h, edge),
        "inner": lambda i, h: pass_on(i, h, inner),
        "wedge": lambda i, p: wide_on(i, p, edge),
        "winner": lambda i, p: wide_on(i, p, inner),
        "cross": wide_across,
        "block": use_block,
        "fin": own_done,
        "finw": wide_done,
    }
    def settle():
        for place in range(half):
            ref = part_recv.at[place]
            remote(ref, ref, send_sem.at[0], part_recv_sem.at[place], rep_peer).wait_recv()
            out_ref[:, place * deep : (place + 1) * deep] = (
                part[rep * half + place] + part_recv[place].astype(jnp.float32)
            ).astype(jnp.bfloat16)
        for make, given in started:
            if given:
                pl.when(functools.reduce(jnp.logical_and, given))(lambda: make().wait_send())
            else:
                make().wait_send()

    for name, *given in ORDER[:-1]:
        acts[name](*given)
    settle()
    for name, *given in ORDER[-1:]:
        acts[name](*given)


def handed_on(values):
    count = len(values)

    def body(*refs):
        sems = refs[-1]
        copies = [
            pltpu.make_async_copy(refs[index], refs[count + index], sems.at[index]) for index in range(count)
        ]
        for copy in copies:
            copy.start()
        for copy in copies:
            copy.wait()

    return pl.pallas_call(
        body,
        out_shape=[jax.ShapeDtypeStruct(value.shape, value.dtype) for value in values],
        in_specs=[pl.BlockSpec(memory_space=pltpu.VMEM)] * count,
        out_specs=[pl.BlockSpec(memory_space=pl.ANY)] * count,
        scratch_shapes=[pltpu.SemaphoreType.DMA((count,))],
        compiler_params=pltpu.CompilerParams(vmem_limit_bytes=8 * 1024 * 1024),
    )(*[pltpu.with_memory_space_constraint(value, pltpu.VMEM) for value in values])


def in_one_kernel(size, gate_pre, up_pre, out_grad, master, moment_one, moment_two):
    micro, count, ff = gate_pre.shape
    tokens, depth, rows = micro * count, out_grad.shape[2], master.shape[0]
    outer = size // (MID * CORES)
    deep = MID * CORES * rows
    split = max(1, round(ff * ALONG / 128)) * 128
    early = max(1, round(ff * ACROSS / LANES)) * LANES
    cot = out_grad.reshape(tokens, depth)
    hbm = pl.BlockSpec(memory_space=pl.ANY)
    bf, f32 = jnp.bfloat16, jnp.float32
    dma = pltpu.SemaphoreType.DMA
    results = pl.pallas_call(
        functools.partial(fused, outer, tokens * size, split, early),
        out_shape=(
            pltpu.VMEM((tokens, depth // 2), bf),
            pltpu.VMEM((tokens, ff), bf),
            pltpu.VMEM((tokens, ff), bf),
            pltpu.VMEM((rows, ff), f32),
            pltpu.VMEM((rows, ff), f32),
            pltpu.VMEM((rows, ff), f32),
        ),
        in_specs=[hbm] * 6,
        out_specs=(pl.BlockSpec(memory_space=pltpu.VMEM),) * 6,
        scratch_shapes=[
            pltpu.VMEM((size, rows, ff), bf),
            pltpu.VMEM((tokens, ff), bf),
            pltpu.VMEM((tokens, ff), bf),
            pltpu.VMEM((MID, outer, rows, tokens), bf),
            pltpu.VMEM((outer, rows, early), f32),
            pltpu.VMEM((outer, rows, early), bf),
            pltpu.VMEM((outer, rows, early), bf),
            pltpu.VMEM((outer, rows, early), bf),
            pltpu.VMEM((2, outer, rows, early), bf),
            pltpu.VMEM((MID, outer, rows, ff - early), f32),
            pltpu.VMEM((MID, outer, rows, ff - early), bf),
            pltpu.VMEM((2, MID, outer, rows, ff - early), bf),
            pltpu.VMEM((rows, ff - early), bf),
            pltpu.VMEM((rows, ff - early), bf),
            pltpu.VMEM((outer, tokens, deep), f32),
            pltpu.VMEM((outer, tokens, deep), bf),
            pltpu.VMEM((outer // 2, tokens, deep), bf),
            pltpu.VMEM((tokens, ff), f32),
            pltpu.VMEM((CORES, MID, outer, rows, tokens), bf),
            pltpu.VMEM((tokens, ff), bf),
            pltpu.VMEM((tokens, ff), bf),
            pltpu.VMEM((tokens, depth), bf),
            pltpu.VMEM((rows, ff), f32),
            pltpu.VMEM((rows, ff), f32),
            pltpu.VMEM((rows, ff), f32),
            dma((6,)), dma((40 * outer,)), dma((2, size)), dma((3,)),
            dma((2, outer)), dma((2, 2, outer)), dma((2, MID, outer)), dma, dma((outer // 2,)),
        ],
        compiler_params=pltpu.CompilerParams(
            collective_id=0, has_side_effects=True, vmem_limit_bytes=50 * 1024 * 1024
        ),
    )(
        gate_pre.reshape(tokens, ff), up_pre.reshape(tokens, ff), cot, master, moment_one, moment_two,
    )
    results = handed_on(results)
    split = [value.reshape(micro, count, value.shape[1]) for value in results[:3]]
    return (*split, *results[3:])


def with_collectives(gate_pre, up_pre, out_grad, master, moment_one, moment_two):
    weights = lax.all_gather(master.astype(jnp.bfloat16), "dp", axis=0, tiled=True)
    micro = gate_pre.shape[0]
    total = micro * gate_pre.shape[1] * lax.axis_size("dp")
    outs_list = []
    gate_list = []
    up_list = []
    grad_sum = None
    for index in range(micro):
        gate = gate_pre[index].astype(jnp.float32)
        up_val = up_pre[index].astype(jnp.float32)
        sig = jax.nn.sigmoid(gate)
        hidden = (gate * sig * up_val).astype(jnp.bfloat16)
        partial_out = lax.dot_general(
            hidden, weights, (((1,), (1,)), ((), ())), preferred_element_type=jnp.float32
        )
        outs_list.append(
            lax.psum_scatter(partial_out, "rep", scatter_dimension=1, tiled=True).astype(
                jnp.bfloat16
            )
        )
        hid_grad = jnp.dot(out_grad[index], weights, preferred_element_type=jnp.float32)
        gate_list.append(
            (hid_grad * up_val * sig * (1.0 + gate * (1.0 - sig))).astype(jnp.bfloat16)
        )
        up_list.append((hid_grad * gate * sig).astype(jnp.bfloat16))
        term = lax.dot_general(
            out_grad[index], hidden, (((0,), (0,)), ((), ())), preferred_element_type=jnp.float32
        )
        shard = lax.psum_scatter(term, "dp", scatter_dimension=0, tiled=True)
        grad_sum = shard if grad_sum is None else grad_sum + shard
    updated = adam(grad_sum / jnp.float32(total), master, moment_one, moment_two)
    return jnp.stack(outs_list), jnp.stack(gate_list), jnp.stack(up_list), *updated


def solution(mesh):
    size = mesh.shape["dp"]

    def on_device(gate_pre, up_pre, out_grad, master, moment_one, moment_two):
        line = size == LINE * MID * CORES
        tall = line and master.shape[0] % 32 == 0 and master.shape[1] % LANES == 0 and master.shape[1] >= 8 * LANES
        step = functools.partial(in_one_kernel, size) if tall else with_collectives
        return step(gate_pre, up_pre, out_grad, master, moment_one, moment_two)

    split = P(None, "dp", "rep")
    owned = P("dp", "rep")
    return jax.shard_map(
        on_device,
        mesh=mesh,
        in_specs=(split, split, P(None, "dp", None), owned, owned, owned),
        out_specs=(split, split, split, owned, owned, owned),
        check_vma=False,
    )
```
